256 devices in a mesh: patch: 64 (over x, z, core), rep: 4 (over y).
Axes of the slice: x: 4, y: 4, z: 8, core: 2. Of those that a mesh axis runs over, the one named last changes fastest.
Arguments:
- node_latents: bfloat16 [4, 24576, 512], P('rep', 'patch'), may hold values from -6 to 6
- edge_latents: bfloat16 [4, 81920, 512], P('rep', 'patch'), may hold values from -6 to 6
- targets: bfloat16 [4, 24576, 128], P('rep', 'patch'), may hold values from -6 to 6
- edge_weight_in: bfloat16 [1536, 512], replicated, may hold values from -0.15625 to 0.15625
- edge_weight_out: bfloat16 [512, 512], replicated, may hold values from -0.25 to 0.25
- node_weight_in: bfloat16 [1024, 512], replicated, may hold values from -0.1875 to 0.1875
- node_weight_out: bfloat16 [512, 512], replicated, may hold values from -0.25 to 0.25
- readout_weight: bfloat16 [512, 128], replicated, may hold values from -0.25 to 0.25
- send_rows: int32 [64, 96], P('patch'), may hold values from 0 to 383, as said below
- far_rows: int32 [64, 64], P('patch'), may hold values from 0 to 383, as said below
- edge_sender: int32 [81920], P('patch'), may hold values from 0 to 543
- edge_receiver: int32 [81920], P('patch'), may hold values from 0 to 383
- edge_count: int32 [64], P('patch'), may hold values from 80 to 1280, as said below
- land_mask: int32 [24576], P('patch'), may hold values 0 or 1
- lat_band: int32 [24576], P('patch'), may hold values from 0 to 720
Outputs:
- node_grad: bfloat16 [4, 24576, 512], P('rep', 'patch')
- edge_grad: bfloat16 [4, 81920, 512], P('rep', 'patch')
- grad_edge_in: float32 [1536, 512], P('patch')
- grad_edge_out: float32 [512, 512], P('patch')
- grad_node_in: float32 [1024, 512], P('patch')
- grad_node_out: float32 [512, 512], P('patch')
- grad_readout: float32 [512, 128], P('patch')
The draws below stay inside these ranges and needn't reach their ends.
Inputs may be any that keep to these rules, and one draw needn't show every extreme that they name: `send_rows`: the 16 entries of a patch for one neighbour are distinct. `far_rows`: each patch sends exactly one node to every patch (itself included). `edge_count`: some patch has all 1280 edges live.
All inputs are finite; a program needn't handle non-finite values. No bound on the sum of `land_mask` on one device may be relied on, other than what follows from the above.
Results may differ from the reference program's by a relative error of at most 0.012.
Values may be sent and summed in bfloat16 or wider, within the bound.
A program may use at most 128 MiB of HBM per device.

```python
import jax
import jax.numpy as jnp
from jax import lax

D = 512
VARS = 128
OCEAN = 32
BANDS = 721
NODE_DEV = 384
EDGE_DEV = 1280
SLOT = 16
FAR = 1
PATCHES = 64
REPS = 4
NODES = 24576
EDGES = 81920


def draw_send_rows(key, part):
    patches = EDGES // EDGE_DEV
    scores = jax.random.randint(key, (patches, 6, NODE_DEV), 0, 1 << 16) * NODE_DEV + jnp.arange(NODE_DEV, dtype=jnp.int32)
    order = jnp.argsort(scores, axis=-1, stable=True)[:, :, :SLOT]
    return order.reshape(patches, 6 * SLOT).astype(jnp.int32)


def draw_far_rows(key, part):
    patches = EDGES // EDGE_DEV
    scores = jax.random.randint(key, (patches, patches, NODE_DEV), 0, 1 << 16) * NODE_DEV + jnp.arange(NODE_DEV, dtype=jnp.int32)
    order = jnp.argsort(scores, axis=-1, stable=True)[:, :, :FAR]
    return order.reshape(patches, patches * FAR).astype(jnp.int32)


def draw_edge_sender(key, part):
    patches = EDGES // EDGE_DEV
    kind = jax.random.randint(jax.random.fold_in(key, 1), (EDGES,), 0, 100)
    local = jax.random.randint(jax.random.fold_in(key, 2), (EDGES,), 0, NODE_DEV)
    near = NODE_DEV + jax.random.randint(jax.random.fold_in(key, 3), (EDGES,), 0, 6 * SLOT)
    far = NODE_DEV + 6 * SLOT + jax.random.randint(jax.random.fold_in(key, 4), (EDGES,), 0, FAR * patches)
    return jnp.where(kind < 72, local, jnp.where(kind < 88, near, far)).astype(jnp.int32)


def draw_edge_count(key, part):
    patches = EDGES // EDGE_DEV
    counts = jax.random.randint(key, (patches,), EDGE_DEV // 16, EDGE_DEV + 1)
    fullest = jax.random.randint(jax.random.fold_in(key, 7), (), 0, patches)
    return jnp.where(jnp.arange(patches) == fullest, EDGE_DEV, counts).astype(jnp.int32)


def with_ends(entries, own_key, least, high):
    dims = entries.shape
    spot = [jax.random.randint(jax.random.fold_in(own_key, axis), (), 0, dims[axis]) for axis in range(len(dims))]
    entries = entries.at[tuple(spot)].set(least)
    longest = dims.index(max(dims))
    spot[longest] = (spot[longest] + 1) % dims[longest]
    return entries.at[tuple(spot)].set(high)


def block_levels(rng, extent, pieces, low, high):
    def one(position, parts):
        draws = jax.random.uniform(jax.random.fold_in(jax.random.fold_in(rng, 6), position), (parts,), jnp.float32, low / len(pieces), high / len(pieces))
        return jnp.repeat(jnp.exp(draws), extent[position] // parts).reshape((-1,) + (1,) * (len(extent) - position - 1))

    factor_of = one(*pieces[0])
    for cut in pieces[1:]:
        factor_of = factor_of * one(*cut)
    return factor_of


def normal_values(stream_key, dims, scale, most, split=(), kind=jnp.bfloat16):
    entries = scale * jax.random.normal(stream_key, dims, jnp.float32)
    if split:
        entries = entries * block_levels(stream_key, dims, split, -0.22, 0.18)
    return jnp.clip(entries, -most, most).astype(kind)


def setup_inputs(seed: int = 0) -> dict:
    key_of = jax.random.split(jax.random.key(seed), 16)
    node_latents = normal_values(key_of[0], (REPS, NODES, D), 1.0, 6.0, ((0, 4), (1, 64)))
    edge_latents = normal_values(key_of[1], (REPS, EDGES, D), 1.0, 6.0, ((0, 4), (1, 64)))
    targets = normal_values(key_of[2], (REPS, NODES, VARS), 1.0, 6.0, ((0, 4), (1, 64)))
    edge_weight_in = normal_values(key_of[3], (3 * D, D), (3 * D) ** -0.5, 0.15625)
    edge_weight_out = normal_values(key_of[4], (D, D), D ** -0.5, 0.25)
    node_weight_in = normal_values(key_of[5], (2 * D, D), (2 * D) ** -0.5, 0.1875)
    node_weight_out = normal_values(key_of[6], (D, D), D ** -0.5, 0.25)
    readout_weight = normal_values(key_of[7], (D, VARS), D ** -0.5, 0.25)
    send_rows = draw_send_rows(jax.random.fold_in(key_of[15], 71), 0)
    far_rows = draw_far_rows(jax.random.fold_in(key_of[15], 71), 0)
    edge_sender = draw_edge_sender(jax.random.fold_in(key_of[15], 71), 0)
    edge_receiver = with_ends(jax.random.randint(key_of[11], (EDGES,), 0, NODE_DEV), jax.random.fold_in(key_of[11], 1), 0, NODE_DEV - 1).astype(jnp.int32)
    edge_count = draw_edge_count(jax.random.fold_in(key_of[15], 71), 0)
    land_mask = with_ends((jax.random.randint(key_of[13], (NODES,), 0, 10) < 3).astype(jnp.int32), jax.random.fold_in(key_of[13], 1), 0, 1)
    lat_band = with_ends(jax.random.randint(key_of[14], (NODES,), 0, BANDS), jax.random.fold_in(key_of[14], 1), 0, BANDS - 1).astype(jnp.int32)
    return {"node_latents": node_latents, "edge_latents": edge_latents, "targets": targets, "edge_weight_in": edge_weight_in, "edge_weight_out": edge_weight_out, "node_weight_in": node_weight_in, "node_weight_out": node_weight_out, "readout_weight": readout_weight, "send_rows": send_rows, "far_rows": far_rows, "edge_sender": edge_sender, "edge_receiver": edge_receiver, "edge_count": edge_count, "land_mask": land_mask, "lat_band": lat_band}


def normalize(values):
    average = lax.optimization_barrier(jnp.mean(values, axis=-1, keepdims=True))
    centred = values - average
    variance = lax.optimization_barrier(jnp.mean(centred * centred, axis=-1, keepdims=True))
    inverse = lax.rsqrt(variance + 1e-05)
    return (centred * inverse, inverse)

def norm_back(gradient, normed, inverse):
    first = lax.optimization_barrier(jnp.mean(gradient, axis=-1, keepdims=True))
    second = lax.optimization_barrier(jnp.mean(gradient * normed, axis=-1, keepdims=True))
    return inverse * (gradient - first - normed * second)

def silu_grad(values):
    logistic = jax.nn.sigmoid(values)
    return logistic * (1.0 + values * (1.0 - logistic))

def product(left, right):
    return jnp.dot(left, right, preferred_element_type=jnp.float32)

def product_left(left, right):
    return jnp.dot(left.T, right, preferred_element_type=jnp.float32)

def product_right(left, right):
    return jnp.dot(left, right.T, preferred_element_type=jnp.float32)

def reference(node_latents, edge_latents, targets, edge_weight_in, edge_weight_out, node_weight_in, node_weight_out, readout_weight, send_rows, far_rows, edge_sender, edge_receiver, edge_count, land_mask, lat_band):
    positions = jnp.arange(EDGES, dtype=jnp.int32)
    device = (positions // EDGE_DEV).astype(jnp.int32)
    near_total = 6 * SLOT
    offset = jnp.maximum(edge_sender - NODE_DEV, 0).astype(jnp.int32)
    near_index = jnp.minimum(offset, near_total - 1).astype(jnp.int32)
    neighbour = (near_index // SLOT).astype(jnp.int32)
    distance = ((neighbour // 2 + 1) * (1 - 2 * (neighbour % 2))).astype(jnp.int32)
    near_patch = ((device - distance + PATCHES) % PATCHES).astype(jnp.int32)
    near_node = near_patch * NODE_DEV + send_rows[near_patch, near_index]
    far_index = jnp.maximum(offset - near_total, 0).astype(jnp.int32)
    far_patch = jnp.minimum(far_index // FAR, PATCHES - 1).astype(jnp.int32)
    far_node = far_patch * NODE_DEV + far_rows[far_patch, device * FAR + far_index % FAR]
    remote = jnp.where(offset < near_total, near_node, far_node)
    senders = jnp.where(edge_sender < NODE_DEV, device * NODE_DEV + edge_sender, remote).astype(jnp.int32)
    receivers = (device * NODE_DEV + edge_receiver).astype(jnp.int32)
    alive_mask = (positions % EDGE_DEV < edge_count[device]).astype(jnp.float32)[:, None]
    latitude = -0.5 * jnp.pi + (lat_band.astype(jnp.float32) + 0.5) * (jnp.pi / BANDS)
    area_weight = jnp.cos(latitude)[:, None]
    channel = jnp.arange(VARS, dtype=jnp.int32)
    keep_mask = jnp.where((channel[None, :] < OCEAN) & (land_mask[:, None] == 1), 0.0, 1.0).astype(jnp.float32)
    loss_weight = area_weight * keep_mask
    sums = [jnp.zeros(w.shape, jnp.float32) for w in (edge_weight_in, edge_weight_out, node_weight_in, node_weight_out, readout_weight)]
    node_grads = []
    edge_grads = []
    for replica in range(REPS):
        node_rows = node_latents[replica]
        edge_rows = edge_latents[replica]
        stacked = jnp.concatenate([node_rows[senders], node_rows[receivers], edge_rows], axis=1)
        edge_pre = product(stacked, edge_weight_in)
        edge_hidden = jax.nn.silu(edge_pre).astype(jnp.bfloat16)
        edge_normed, edge_inverse = normalize(product(edge_hidden, edge_weight_out))
        message = (edge_normed * alive_mask).astype(jnp.bfloat16)
        aggregate = jax.ops.segment_sum(message.astype(jnp.float32), receivers, num_segments=NODES).astype(jnp.bfloat16)
        node_input = jnp.concatenate([node_rows, aggregate], axis=1)
        node_pre = product(node_input, node_weight_in)
        node_hidden = jax.nn.silu(node_pre).astype(jnp.bfloat16)
        node_normed, node_inverse = normalize(product(node_hidden, node_weight_out))
        updated = (node_rows.astype(jnp.float32) + node_normed).astype(jnp.bfloat16)
        predicted = product(updated, readout_weight)
        pred_grad = (loss_weight * (predicted - targets[replica].astype(jnp.float32))).astype(jnp.bfloat16)
        updated_grad = product_right(pred_grad, readout_weight)
        node_z_grad = norm_back(updated_grad, node_normed, node_inverse).astype(jnp.bfloat16)
        node_pre_grad = (product_right(node_z_grad, node_weight_out) * silu_grad(node_pre)).astype(jnp.bfloat16)
        input_grad = product_right(node_pre_grad, node_weight_in)
        message_grad = input_grad[:, D:][receivers] * alive_mask
        edge_z_grad = norm_back(message_grad, edge_normed, edge_inverse).astype(jnp.bfloat16)
        edge_pre_grad = (product_right(edge_z_grad, edge_weight_out) * silu_grad(edge_pre)).astype(jnp.bfloat16)
        stacked_grad = product_right(edge_pre_grad, edge_weight_in)
        sender_grad = stacked_grad[:, :D].astype(jnp.bfloat16).astype(jnp.float32)
        receiver_grad = stacked_grad[:, D:2 * D].astype(jnp.bfloat16).astype(jnp.float32)
        edge_grads.append(stacked_grad[:, 2 * D:].astype(jnp.bfloat16))
        total = updated_grad + input_grad[:, :D]
        total = total + jax.ops.segment_sum(sender_grad, senders, num_segments=NODES)
        total = total + jax.ops.segment_sum(receiver_grad, receivers, num_segments=NODES)
        node_grads.append(total.astype(jnp.bfloat16))
        sums[0] = sums[0] + product_left(stacked, edge_pre_grad)
        sums[1] = sums[1] + product_left(edge_hidden, edge_z_grad)
        sums[2] = sums[2] + product_left(node_input, node_pre_grad)
        sums[3] = sums[3] + product_left(node_hidden, node_z_grad)
        sums[4] = sums[4] + product_left(updated, pred_grad)
    factor = 1.0 / (NODES * REPS)
    return (jnp.stack(node_grads), jnp.stack(edge_grads), sums[0] * factor, sums[1] * factor, sums[2] * factor, sums[3] * factor, sums[4] * factor)
```

```python
import functools

import jax
import jax.numpy as jnp
from jax import lax
from jax.experimental import pallas as pl
from jax.experimental.pallas import tpu as pltpu
from jax.sharding import Mesh
from jax.sharding import PartitionSpec as P

OCEAN = 32
BANDS = 721
PATCH = ("patch_0", "patch_1", "patch_2")
MESH = pl.DeviceIdType.MESH
D = 512
NODE = 384
EDGE = 1280
NEAR = 96
FAR = 64
EXT = 640
TABLE = EXT + NODE
TILE = 256
OFFSETS = (1, -1, 2, -2, 3, -3)
BF = jnp.bfloat16
F32 = jnp.float32


def dot(a, b):
    return jnp.dot(a, b, preferred_element_type=F32)


def dot_t(a, b):
    return lax.dot_general(a, b, (((1,), (1,)), ((), ())), preferred_element_type=F32)


def t_dot(a, b):
    return lax.dot_general(a, b, (((0,), (0,)), ((), ())), preferred_element_type=F32)


def patch_id(q):
    return {"patch_0": q // 16, "patch_1": (q // 2) % 8, "patch_2": q % 2}


def normalize(v):
    mean = jnp.mean(v, axis=-1, keepdims=True)
    centred = v - mean
    var = jnp.mean(centred * centred, axis=-1, keepdims=True)
    inverse = lax.rsqrt(var + 1e-05)
    return centred * inverse, inverse


def norm_back(g, y, inverse):
    first = jnp.mean(g, axis=-1, keepdims=True)
    second = jnp.mean(g * y, axis=-1, keepdims=True)
    return inverse * (g - first - y * second)


def columns(rows):
    wide = rows[0].shape[1]
    pad = [jnp.zeros((8 - len(rows), wide), F32)]
    return jnp.concatenate(rows + pad, axis=0).T


class Reducer:
    def __init__(self, refs, where):
        (self.start0, self.r0, self.w1, self.r1, self.w2, self.r2, self.w3,
         self.r3, self.w4, self.r4, self.send, self.recv) = refs
        self.x, self.y, self.z, self.c = where
        self.pending = []

    def copy(self, src, dst, k, device):
        one = pltpu.make_async_remote_copy(
            src_ref=src, dst_ref=dst, send_sem=self.send.at[k], recv_sem=self.recv.at[k],
            device_id=device, device_id_type=MESH,
        )
        one.start()
        self.pending.append(one)
        return one

    def pair(self):
        other = 1 - self.c
        self.c0 = [
            self.copy(self.start0.at[h, other], self.r0.at[h], h, {"patch_2": other})
            for h in range(2)
        ]

    def over_x(self, src, dst, k):
        out = []
        for d in range(1, 4):
            to = (self.x + d) % 4
            out.append(self.copy(src(to), dst(d - 1), k + d - 1, {"patch_0": to}))
        return out

    def over_y(self, src, dst, k):
        out = []
        for d in range(1, 4):
            to = (self.y + d) % 4
            out.append(self.copy(src(to), dst(d - 1), k + d - 1, {"rep": to}))
        return out

    def first(self):
        for h in range(2):
            self.c0[h].wait_recv()

            @pl.loop(0, 4)
            def _(i):
                mine = self.start0[h, self.c, i].astype(F32)
                self.w1[h, i] = (mine + self.r0[h, i].astype(F32)).astype(BF)

            if h == 0:
                self.c1a = self.over_x(lambda to: self.w1.at[0, to], lambda s: self.r1.at[0, s], 2)
            else:
                self.c1b = self.over_y(
                    lambda to: self.w1.at[1, :, to],
                    lambda s: self.r1.at[1, s],
                    5,
                )

    def second(self):
        for one in self.c1a:
            one.wait_recv()

        @pl.loop(0, 4)
        def _(y):
            acc = self.w1[0, self.x, y].astype(F32)
            for s in range(3):
                acc = acc + self.r1[0, s, y].astype(F32)
            self.w2[0, y] = acc.astype(BF)

        self.c2a = self.over_y(lambda to: self.w2.at[0, to], lambda s: self.r2.at[0, s], 8)
        for one in self.c1b:
            one.wait_recv()

        @pl.loop(0, 4)
        def _(i):
            acc = self.w1[1, i, self.y].astype(F32)
            for s in range(3):
                acc = acc + self.r1[1, s, i].astype(F32)
            self.w2[1, i] = acc.astype(BF)

        self.c2b = self.over_x(lambda to: self.w2.at[1, to], lambda s: self.r2.at[1, s], 11)

    def third(self):
        for h, (copies, mine) in enumerate(((self.c2a, self.y), (self.c2b, self.x))):
            for one in copies:
                one.wait_recv()
            acc = self.w2[h, mine].astype(F32)
            for s in range(3):
                acc = acc + self.r2[h, s].astype(F32)
            self.w3[:, h] = acc.astype(BF)
        self.c3 = []
        for d in range(1, 8):
            to = (self.z + d) % 8
            self.c3.append(self.copy(self.w3.at[to], self.r3.at[d - 1], 13 + d, {"patch_1": to}))

    def fourth(self):
        for one in self.c3:
            one.wait_recv()
        acc = self.w3[self.z].astype(F32)
        for s in range(7):
            acc = acc + self.r3[s].astype(F32)
        self.w4[...] = acc * (1.0 / (NODE * 64 * 4))
        self.c4 = []
        for d in range(1, 4):
            to = (self.y + d) % 4
            self.c4.append(self.copy(self.w4, self.r4.at[d - 1], 20 + d, {"rep": to}))

    def last(self):
        for one in self.c4:
            one.wait_recv()
        out = []
        own = self.w4[...]
        got = [self.r4[s] for s in range(3)]
        for y in range(4):
            tile = own
            for s in range(3):
                tile = jnp.where((self.y - s - 1 + 4) % 4 == y, got[s], tile)
            out.append(tile)
        return out

    def finish(self):
        for one in self.pending:
            one.wait_send()


def kernel(
    x_hbm, e_hbm, t_hbm, we_in_hbm, we_out_hbm, wn_in_hbm, wn_out_hbm, wr_hbm,
    send_ref, far_ref, sender_ref, receiver_ref, count_ref, land_ref, lat_ref,
    node_out, edge_out, gei_out, geo_out, gni_out, gno_out, gr_out,
    xe, e, tgt, we_in, we_out, wn_in, wn_out, wr, edge_res,
    near_src, near_got, far_src, far_got, back_near_src, back_near_got, back_far_src, back_far_got,
    onehot, onehot_t, own_near, own_far, proj, pre, hid, slope, msg, inv, ezg, epg, total, agg_grad, gsum, wgrad,
    *rest,
):
    dma_sem, out_sem, near_send, near_recv, far_send, far_recv = rest[:6]
    bnear_send, bnear_recv, bfar_send, bfar_recv = rest[6:10]
    group_a, group_b = rest[10:22], rest[22:34]
    ix, iz, ic, iy = (lax.axis_index(a) for a in (*PATCH, "rep"))
    me = ix * 16 + iz * 2 + ic

    loads = {}
    for k, (name, src, dst) in enumerate((
        ("x", x_hbm.at[0], xe.at[pl.ds(0, NODE)]),
        ("we_in", we_in_hbm, we_in),
        ("e", e_hbm.at[0], e),
        ("we_out", we_out_hbm, we_out),
        ("wn_in", wn_in_hbm, wn_in),
        ("wn_out", wn_out_hbm, wn_out),
        ("wr", wr_hbm, wr),
        ("t", t_hbm.at[0], tgt),
    )):
        loads[name] = pltpu.make_async_copy(src, dst, dma_sem.at[k])
        loads[name].start()

    barrier = pltpu.get_barrier_semaphore()

    @pl.loop(1, 64)
    def _(d):
        pl.semaphore_signal(barrier, inc=1, device_id=patch_id((me + d) % 64), device_id_type=MESH)

    for d in range(1, 4):
        pl.semaphore_signal(
            barrier, inc=1, device_id={"rep": (iy + d) % 4}, device_id_type=MESH
        )

    ids = lax.broadcasted_iota(jnp.int32, (NODE, NEAR), 0)
    own_near[...] = jnp.where(ids == send_ref[...], 1.0, 0.0).astype(BF)
    ids = lax.broadcasted_iota(jnp.int32, (NODE, FAR), 0)
    own_far[...] = jnp.where(ids == far_ref[...], 1.0, 0.0).astype(BF)
    loads["x"].wait()
    x = xe[pl.ds(0, NODE), :]
    near_src[...] = t_dot(own_near[...], x).astype(BF).reshape(6, 16, D)
    far_src[...] = t_dot(own_far[...], x).reshape(FAR, 1, D)

    spot = lax.broadcasted_iota(jnp.int32, (1, EDGE), 1)
    live = spot < count_ref[...]
    s_row = jnp.where(live, sender_ref[...], -1)
    r_row = jnp.where(live, receiver_ref[...] + EXT, -1)
    cols = columns([s_row.astype(F32), r_row.astype(F32)])
    s_col = cols[:, 0:1].astype(jnp.int32)
    r_col = cols[:, 1:2].astype(jnp.int32)
    for k in range(TABLE // 128):
        ids = lax.broadcasted_iota(jnp.int32, (EDGE, 128), 1) + k * 128
        which = s_col if k < EXT // 128 else r_col
        onehot[:, pl.ds(k * 128, 128)] = jnp.where(ids == which, 1.0, 0.0).astype(BF)
    for k in range(TABLE // 128):
        ids = lax.broadcasted_iota(jnp.int32, (128, EDGE), 0) + k * 128
        which = s_row if k < EXT // 128 else r_row
        onehot_t[pl.ds(k * 128, 128), :] = jnp.where(ids == which, 1.0, 0.0).astype(BF)

    pl.semaphore_wait(barrier, 66)

    nears = []
    for k, o in enumerate(OFFSETS):
        one = pltpu.make_async_remote_copy(
            src_ref=near_src.at[k], dst_ref=near_got.at[k],
            send_sem=near_send.at[k], recv_sem=near_recv.at[k],
            device_id=patch_id((me + o + 64) % 64), device_id_type=MESH,
        )
        one.start()
        nears.append(one)

    def far_copy(src, dst, send, recv, d):
        to = (me + d) % 64
        return pltpu.make_async_remote_copy(
            src_ref=src.at[to], dst_ref=dst.at[me], send_sem=send, recv_sem=recv,
            device_id=patch_id(to), device_id_type=MESH,
        )

    @pl.loop(1, 64)
    def _(d):
        far_copy(far_src, far_got, far_send.at[0], far_recv.at[0], d).start()

    def far_wait(src, dst, send, recv):
        all_of = pltpu.make_async_remote_copy(
            src_ref=src.at[pl.ds(0, 63)], dst_ref=dst.at[pl.ds(0, 63)],
            send_sem=send, recv_sem=recv,
            device_id=patch_id((me + 1) % 64), device_id_type=MESH,
        )
        return all_of

    loads["we_in"].wait()
    proj[pl.ds(0, NODE), :] = dot(x, we_in[pl.ds(0, D), :]).astype(BF)
    proj[pl.ds(EXT, NODE), :] = dot(x, we_in[pl.ds(D, D), :]).astype(BF)
    loads["e"].wait()
    pre[...] = dot(e[...], we_in[pl.ds(2 * D, D), :])

    for one in nears:
        one.wait_recv()
    far_all = far_wait(far_src, far_got, far_send.at[0], far_recv.at[0])
    far_all.wait_recv()
    xe[pl.ds(NODE, NEAR), :] = near_got[...].reshape(NEAR, D)
    slot = lax.broadcasted_iota(jnp.int32, (FAR, 1), 0)
    far_rows = jnp.where(slot == me, far_src[...].reshape(FAR, D), far_got[...].reshape(FAR, D))
    xe[pl.ds(NODE + NEAR, FAR), :] = far_rows.astype(BF)
    xe[pl.ds(NODE + NEAR + FAR, 96), :] = jnp.zeros((96, D), BF)
    proj[pl.ds(NODE, EXT - NODE), :] = dot(
        xe[pl.ds(NODE, EXT - NODE), :], we_in[pl.ds(0, D), :]
    ).astype(BF)

    loads["we_out"].wait()

    @pl.loop(0, EDGE // TILE)
    def _(k):
        at = pl.ds(pl.multiple_of(k * TILE, TILE), TILE)
        v = pre[at, :] + dot(onehot[at, :], proj[...])
        s = jax.nn.sigmoid(v)
        h = (v * s).astype(BF)
        hid[at, :] = h
        slope[at, :] = s * (1.0 + v * (1.0 - s))
        normed, inverse = normalize(dot(h, we_out[...]))
        msg[at, :] = normed.astype(BF)
        inv[at, :] = jnp.broadcast_to(inverse, (TILE, 128))

    aggregate = dot(onehot_t[pl.ds(EXT, NODE), :], msg[...]).astype(BF)

    loads["wn_in"].wait()
    node_pre = dot(x, wn_in[pl.ds(0, D), :]) + dot(aggregate, wn_in[pl.ds(D, D), :])
    s = jax.nn.sigmoid(node_pre)
    node_hidden = (node_pre * s).astype(BF)
    node_slope = s * (1.0 + node_pre * (1.0 - s))
    loads["wn_out"].wait()
    node_normed, node_inverse = normalize(dot(node_hidden, wn_out[...]))
    updated = (x.astype(F32) + node_normed).astype(BF)
    loads["wr"].wait()
    predicted = dot(updated, wr[...])
    latitude = -0.5 * jnp.pi + (lat_ref[...].astype(F32) + 0.5) * (jnp.pi / BANDS)
    cols = columns([jnp.cos(latitude), land_ref[...].astype(F32)])
    area, land = cols[:, 0:1], cols[:, 1:2]
    channel = lax.broadcasted_iota(jnp.int32, (NODE, 128), 1)
    weight = jnp.where((channel < OCEAN) & (land == 1.0), 0.0, area)
    loads["t"].wait()
    pred_grad = (weight * (predicted - tgt[...].astype(F32))).astype(BF)
    updated_grad = dot_t(pred_grad, wr[...])
    node_z_grad = norm_back(updated_grad, node_normed, node_inverse).astype(BF)
    node_pre_grad = (dot_t(node_z_grad, wn_out[...]) * node_slope).astype(BF)
    total[...] = updated_grad + dot_t(node_pre_grad, wn_in[pl.ds(0, D), :])
    agg_grad[...] = dot_t(node_pre_grad, wn_in[pl.ds(D, D), :]).astype(BF)

    where = (ix, iy, iz, ic)
    ga, gb = Reducer(group_a, where), Reducer(group_b, where)

    def pack_rows(start0, value, blocks, slots):
        rows = value.reshape(4, 8, 2, blocks, 8, D)
        for b, (h, t) in enumerate(slots):
            for c in range(2):
                for y in range(4):
                    tile = rows[:, :, c, b, :, y * 128 : (y + 1) * 128].astype(BF)
                    start0[h, c, :, y, :, t] = tile

    wgrad[pl.ds(0, D), :] = t_dot(x, node_pre_grad)
    wgrad[pl.ds(D, D), :] = t_dot(aggregate, node_pre_grad)
    pack_rows(ga.start0, wgrad[pl.ds(0, 2 * D), :], 2, ((0, 0), (0, 1)))
    pack_rows(ga.start0, t_dot(node_hidden, node_z_grad), 1, ((1, 0),))
    readout = t_dot(updated, pred_grad).reshape(4, 8, 2, 8, 128)
    for c in range(2):
        for y in range(4):
            ga.start0[1, c, :, y, :, 1] = readout[:, :, c].astype(BF)
    ga.pair()

    @pl.loop(0, EDGE // TILE)
    def _(k):
        at = pl.ds(pl.multiple_of(k * TILE, TILE), TILE)
        g = dot(onehot[at, pl.ds(EXT, NODE)], agg_grad[...])
        z_grad = norm_back(g, msg[at, :].astype(F32), inv[at, :][:, 0:1]).astype(BF)
        ezg[at, :] = z_grad
        epg[at, :] = (dot_t(z_grad, we_out[...]) * slope[at, :]).astype(BF)

    ga.first()
    gsum[...] = dot(onehot_t[...], epg[...]).astype(BF)

    back = dot_t(gsum[pl.ds(NODE, EXT - NODE), :], we_in[pl.ds(0, D), :])
    back_near_src[...] = back[0:NEAR].astype(BF).reshape(6, 16, D)
    back_far_src[...] = back[NEAR : NEAR + FAR].reshape(FAR, 1, D)
    backs = []
    for k, o in enumerate(OFFSETS):
        one = pltpu.make_async_remote_copy(
            src_ref=back_near_src.at[k], dst_ref=back_near_got.at[k],
            send_sem=bnear_send.at[k], recv_sem=bnear_recv.at[k],
            device_id=patch_id((me - o + 64) % 64), device_id_type=MESH,
        )
        one.start()
        backs.append(one)

    @pl.loop(1, 64)
    def _(d):
        far_copy(back_far_src, back_far_got, bfar_send.at[0], bfar_recv.at[0], d).start()

    wgrad[pl.ds(0, D), :] = t_dot(xe[...], gsum[pl.ds(0, EXT), :])
    wgrad[pl.ds(D, D), :] = t_dot(x, gsum[pl.ds(EXT, NODE), :])
    wgrad[pl.ds(2 * D, D), :] = t_dot(e[...], epg[...])
    pack_rows(gb.start0, wgrad[...], 3, ((0, 0), (0, 1), (1, 0)))
    pack_rows(gb.start0, t_dot(hid[...], ezg[...]), 1, ((1, 1),))
    gb.pair()
    ga.second()

    edge_res[...] = dot_t(epg[...], we_in[pl.ds(2 * D, D), :]).astype(BF)
    edge_copy = pltpu.make_async_copy(edge_res, edge_out.at[0], out_sem.at[0])
    edge_copy.start()
    gb.first()
    total[...] += dot_t(gsum[pl.ds(0, NODE), :], we_in[pl.ds(0, D), :]) + dot_t(
        gsum[pl.ds(EXT, NODE), :], we_in[pl.ds(D, D), :]
    )
    ga.third()
    gb.second()
    ga.fourth()

    for one in backs:
        one.wait_recv()
    back_all = far_wait(back_far_src, back_far_got, bfar_send.at[0], bfar_recv.at[0])
    back_all.wait_recv()
    far_rows = jnp.where(
        slot == me, back_far_src[...].reshape(FAR, D), back_far_got[...].reshape(FAR, D)
    ).astype(BF)
    owned = dot(own_near[...], back_near_got[...].reshape(NEAR, D)) + dot(own_far[...], far_rows)
    node_out[0] = (total[...] + owned).astype(BF)

    gb.third()
    parts = ga.last()
    for y in range(4):
        at = pl.ds(y * 128, 128)
        gni_out[pl.ds(0, 8), at] = parts[y][0, 0]
        gni_out[pl.ds(8, 8), at] = parts[y][0, 1]
        gno_out[:, at] = parts[y][1, 0]
    gr_out[...] = parts[0][1, 1]
    gb.fourth()
    parts = gb.last()
    for y in range(4):
        at = pl.ds(y * 128, 128)
        gei_out[pl.ds(0, 8), at] = parts[y][0, 0]
        gei_out[pl.ds(8, 8), at] = parts[y][0, 1]
        gei_out[pl.ds(16, 8), at] = parts[y][1, 0]
        geo_out[:, at] = parts[y][1, 1]

    edge_copy.wait()
    for one in nears + backs:
        one.wait_send()
    far_all.wait_send()
    back_all.wait_send()
    ga.finish()
    gb.finish()


def group_scratch():
    tail = (8, 128)
    return [
        pltpu.VMEM((2, 2, 4, 4, 8, 2, *tail), BF),
        pltpu.VMEM((2, 4, 4, 8, 2, *tail), BF),
        pltpu.VMEM((2, 4, 4, 8, 2, *tail), BF),
        pltpu.VMEM((2, 3, 4, 8, 2, *tail), BF),
        pltpu.VMEM((2, 4, 8, 2, *tail), BF),
        pltpu.VMEM((2, 3, 8, 2, *tail), BF),
        pltpu.VMEM((8, 2, 2, *tail), BF),
        pltpu.VMEM((7, 2, 2, *tail), BF),
        pltpu.VMEM((2, 2, *tail), F32),
        pltpu.VMEM((3, 2, 2, *tail), F32),
        pltpu.SemaphoreType.DMA((24,)),
        pltpu.SemaphoreType.DMA((24,)),
    ]


def body(*args):
    (x, e, t, we_in, we_out, wn_in, wn_out, wr, send, far, sender, receiver, count, land, lat) = args
    anywhere = pl.BlockSpec(memory_space=pl.ANY)
    vmem = pl.BlockSpec(memory_space=pltpu.VMEM)
    near = pltpu.VMEM((6, 16, D), BF)
    row = pltpu.VMEM((FAR, 1, D), F32)
    sem = pltpu.SemaphoreType.DMA
    scratch = [
        pltpu.VMEM((EXT, D), BF),
        pltpu.VMEM((EDGE, D), BF),
        pltpu.VMEM((NODE, 128), BF),
        pltpu.VMEM((3 * D, D), BF),
        pltpu.VMEM((D, D), BF),
        pltpu.VMEM((2 * D, D), BF),
        pltpu.VMEM((D, D), BF),
        pltpu.VMEM((D, 128), BF),
        pltpu.VMEM((EDGE, D), BF),
        near, near, row, row, near, near, row, row,
        pltpu.VMEM((EDGE, TABLE), BF),
        pltpu.VMEM((TABLE, EDGE), BF),
        pltpu.VMEM((NODE, NEAR), BF),
        pltpu.VMEM((NODE, FAR), BF),
        pltpu.VMEM((TABLE, D), BF),
        pltpu.VMEM((EDGE, D), F32),
        pltpu.VMEM((EDGE, D), BF),
        pltpu.VMEM((EDGE, D), F32),
        pltpu.VMEM((EDGE, D), BF),
        pltpu.VMEM((EDGE, 128), F32),
        pltpu.VMEM((EDGE, D), BF),
        pltpu.VMEM((EDGE, D), BF),
        pltpu.VMEM((NODE, D), F32),
        pltpu.VMEM((NODE, D), BF),
        pltpu.VMEM((TABLE, D), BF),
        pltpu.VMEM((3 * D, D), F32),
        sem((8,)), sem((1,)),
        sem((6,)), sem((6,)), sem((1,)), sem((1,)),
        sem((6,)), sem((6,)), sem((1,)), sem((1,)),
    ] + group_scratch() + group_scratch()
    return pl.pallas_call(
        kernel,
        out_shape=(
            jax.ShapeDtypeStruct((1, NODE, D), BF),
            jax.ShapeDtypeStruct((1, EDGE, D), BF),
            jax.ShapeDtypeStruct((24, D), F32),
            jax.ShapeDtypeStruct((8, D), F32),
            jax.ShapeDtypeStruct((16, D), F32),
            jax.ShapeDtypeStruct((8, D), F32),
            jax.ShapeDtypeStruct((8, 128), F32),
        ),
        in_specs=[anywhere] * 8 + [vmem] * 7,
        out_specs=(vmem, anywhere, vmem, vmem, vmem, vmem, vmem),
        scratch_shapes=scratch,
        compiler_params=pltpu.CompilerParams(
            collective_id=0, has_side_effects=True, vmem_limit_bytes=62 * 1024 * 1024
        ),
    )(
        x, e, t, we_in, we_out, wn_in, wn_out, wr, send, far,
        sender.reshape(1, EDGE), receiver.reshape(1, EDGE), count.reshape(1, 1),
        land.reshape(1, NODE), lat.reshape(1, NODE),
    )


def solution(mesh):
    split = Mesh(
        mesh.devices.reshape(4, 8, 2, mesh.shape["rep"]), ("patch_0", "patch_1", "patch_2", "rep")
    )
    in_specs = (
        P("rep", PATCH, None),
        P("rep", PATCH, None),
        P("rep", PATCH, None),
        P(),
        P(),
        P(),
        P(),
        P(),
        P(PATCH, None),
        P(PATCH, None),
        P(PATCH),
        P(PATCH),
        P(PATCH),
        P(PATCH),
        P(PATCH),
    )
    out_specs = (
        P("rep", PATCH, None),
        P("rep", PATCH, None),
        P(PATCH, None),
        P(PATCH, None),
        P(PATCH, None),
        P(PATCH, None),
        P(PATCH, None),
    )
    return jax.shard_map(body, mesh=split, in_specs=in_specs, out_specs=out_specs, check_vma=False)
```

```python
import functools

import jax
import jax.numpy as jnp
from jax import lax
from jax.experimental import pallas as pl
from jax.experimental.pallas import tpu as pltpu
from jax.sharding import Mesh
from jax.sharding import PartitionSpec as P

OCEAN = 32
BANDS = 721
PATCH = ("patch_0", "patch_1", "patch_2")
MESH = pl.DeviceIdType.MESH
D = 512
NODE = 384
EDGE = 1280
NEAR = 96
FAR = 64
EXT = 640
GOT = EXT - NODE
TABLE = EXT + NODE
TILE = 256
OFFSETS = (1, -1, 2, -2, 3, -3)
BF = jnp.bfloat16
F32 = jnp.float32


def dot(a, b):
    return jnp.dot(a, b, preferred_element_type=F32)


def dot_t(a, b):
    return lax.dot_general(a, b, (((1,), (1,)), ((), ())), preferred_element_type=F32)


def t_dot(a, b):
    return lax.dot_general(a, b, (((0,), (0,)), ((), ())), preferred_element_type=F32)


def patch_id(q):
    return {"patch_0": q // 16, "patch_1": (q // 2) % 8, "patch_2": q % 2}


def greet(barrier, device):
    pl.semaphore_signal(barrier, inc=1, device_id=device, device_id_type=MESH)


def normalize(v):
    mean = jnp.mean(v, axis=-1, keepdims=True)
    centred = v - mean
    var = jnp.mean(centred * centred, axis=-1, keepdims=True)
    inverse = lax.rsqrt(var + 1e-05)
    return centred * inverse, inverse


def norm_back(g, y, inverse):
    first = jnp.mean(g, axis=-1, keepdims=True)
    second = jnp.mean(g * y, axis=-1, keepdims=True)
    return inverse * (g - first - y * second)


def columns(rows):
    wide = rows[0].shape[1]
    pad = [jnp.zeros((8 - len(rows), wide), F32)]
    return jnp.concatenate(rows + pad, axis=0).T


class Reducer:
    def __init__(self, refs, where):
        (self.start0, self.r0, self.w1, self.direct, self.relay, self.merged, self.carried,
         self.w2, self.r2, self.w3, self.r3, self.w4, self.r4, self.send, self.recv) = refs
        x, self.y, self.z, self.c = where
        self.axes = ((("patch_0", x), ("rep", self.y)), (("rep", self.y), ("patch_0", x)))
        self.pending = []

    def copy(self, src, dst, k, device):
        one = pltpu.make_async_remote_copy(
            src_ref=src, dst_ref=dst, send_sem=self.send.at[k], recv_sem=self.recv.at[k],
            device_id=device, device_id_type=MESH,
        )
        one.start()
        self.pending.append(one)
        return one

    def pair(self):
        other = 1 - self.c
        self.c0 = [
            self.copy(self.start0.at[h, other], self.r0.at[h], h, {"patch_2": other})
            for h in range(2)
        ]

    def first(self):
        self.c1 = []
        for h in range(2):
            self.c0[h].wait_recv()

            @pl.loop(0, 4)
            def _(i):
                mine = self.start0[h, self.c, i].astype(F32)
                self.w1[h, i] = (mine + self.r0[h, i].astype(F32)).astype(BF)

            axis, at = self.axes[h][0]
            right, left, across = (at + 1) % 4, (at + 3) % 4, (at + 2) % 4
            lo, hi = pl.ds(0, 2), pl.ds(2, 2)
            w1, k = self.w1, 2 + 6 * h
            self.c1.append((
                self.copy(w1.at[h, across, lo], self.relay.at[h, 0], k, {axis: right}),
                self.copy(w1.at[h, across, hi], self.relay.at[h, 1], k + 1, {axis: left}),
                self.copy(w1.at[h, left, lo], self.direct.at[h, 0], k + 2, {axis: left}),
                self.copy(w1.at[h, right, hi], self.direct.at[h, 1], k + 3, {axis: right}),
            ))

    def middle(self):
        self.c1b = []
        for h in range(2):
            axis, at = self.axes[h][0]
            ends = ((at + 1) % 4, (at + 3) % 4)
            for side in range(2):
                self.c1[h][side].wait_recv()
                mine = self.w1[h, ends[side], pl.ds(2 * side, 2)].astype(F32)
                self.merged[h, side] = (mine + self.relay[h, side].astype(F32)).astype(BF)
                self.c1b.append(self.copy(
                    self.merged.at[h, side], self.carried.at[h, side], 6 + 6 * h + side,
                    {axis: ends[side]},
                ))

    def second(self):
        self.c2 = []
        for h in range(2):
            _, own = self.axes[h][0]
            for side in range(2):
                self.c1[h][2 + side].wait_recv()
                self.c1b[2 * h + side].wait_recv()
                part = pl.ds(2 * side, 2)
                acc = self.w1[h, own, part].astype(F32) + self.direct[h, side].astype(F32)
                self.w2[h, part] = (acc + self.carried[h, side].astype(F32)).astype(BF)
            axis, at = self.axes[h][1]
            for d in range(1, 4):
                to = (at + d) % 4
                self.c2.append(
                    self.copy(self.w2.at[h, to], self.r2.at[h, d - 1], 13 + 3 * h + d, {axis: to})
                )

    def third(self):
        for h in range(2):
            for one in self.c2[3 * h : 3 * h + 3]:
                one.wait_recv()
            acc = self.w2[h, self.axes[h][1][1]].astype(F32)
            for s in range(3):
                acc = acc + self.r2[h, s].astype(F32)
            self.w3[:, h] = acc.astype(BF)
        self.c3 = []
        for d in range(1, 8):
            to = (self.z + d) % 8
            self.c3.append(self.copy(self.w3.at[to], self.r3.at[d - 1], 19 + d, {"patch_1": to}))

    def fourth(self):
        for one in self.c3:
            one.wait_recv()
        acc = self.w3[self.z].astype(F32)
        for s in range(7):
            acc = acc + self.r3[s].astype(F32)
        self.w4[...] = acc * (1.0 / (NODE * 64 * 4))
        self.c4 = []
        for d in range(1, 4):
            to = (self.y + d) % 4
            self.c4.append(self.copy(self.w4, self.r4.at[d - 1], 26 + d, {"rep": to}))

    def last(self):
        for one in self.c4:
            one.wait_recv()
        out = []
        own = self.w4[...]
        got = [self.r4[s] for s in range(3)]
        for y in range(4):
            tile = own
            for s in range(3):
                tile = jnp.where((self.y - s - 1 + 4) % 4 == y, got[s], tile)
            out.append(tile)
        return out

    def finish(self):
        for one in self.pending:
            one.wait_send()


def kernel(
    x_hbm, e_hbm, t_hbm, we_in_hbm, we_out_hbm, wn_in_hbm, wn_out_hbm, wr_hbm,
    send_hbm, far_hbm, sender_hbm, receiver_hbm, count_ref, land_hbm, lat_hbm,
    node_out, edge_out, grads_out,
    send_ref, far_ref, sender_ref, receiver_ref, land_ref, lat_ref,
    xe, e, tgt, we_in, we_out, wn_in, wn_out, wr, edge_res,
    near_src, near_got, far_src, far_got, back_near_src, back_near_got, back_far_src, back_far_mid, back_far_got,
    onehot, onehot_t, own_near, own_far, proj, pre, hid, msg, inv, ezg, epg, total, agg_grad, gsum, wgrad, node_res, grads,
    *rest,
):
    dma_sem, out_sem, near_send, near_recv, far_send, far_recv = rest[:6]
    bnear_send, bnear_recv, bfar_send, bfar_recv = rest[6:10]
    group_a, group_b = rest[10:25], rest[25:40]
    ix, iz, ic, iy = (lax.axis_index(a) for a in (*PATCH, "rep"))
    me = ix * 16 + iz * 2 + ic

    loads = {}
    for k, (name, src, dst) in enumerate((
        ("send", send_hbm, send_ref),
        ("far", far_hbm, far_ref),
        ("sender", sender_hbm, sender_ref),
        ("receiver", receiver_hbm, receiver_ref),
        ("x", x_hbm.at[0], xe.at[pl.ds(GOT, NODE)]),
        ("we_in", we_in_hbm, we_in),
        ("e", e_hbm.at[0], e),
        ("we_out", we_out_hbm, we_out),
        ("wn_in", wn_in_hbm, wn_in),
        ("wn_out", wn_out_hbm, wn_out),
        ("wr", wr_hbm, wr),
        ("t", t_hbm.at[0], tgt),
        ("land", land_hbm, land_ref),
        ("lat", lat_hbm, lat_ref),
    )):
        loads[name] = pltpu.make_async_copy(src, dst, dma_sem.at[k])
        loads[name].start()

    barrier = pltpu.get_barrier_semaphore()

    @pl.loop(0, 63, unroll=7)
    def _(k):
        greet(barrier, patch_id((me + 1 + (k + 32) % 63) % 64))

    for d in range(1, 4):
        greet(barrier, {"rep": (iy + d) % 4})

    loads["send"].wait()
    loads["far"].wait()
    ids = lax.broadcasted_iota(jnp.int32, (NODE, NEAR), 0)
    own_near[...] = jnp.where(ids == send_ref[...], 1.0, 0.0).astype(BF)
    ids = lax.broadcasted_iota(jnp.int32, (NODE, FAR), 0)
    own_far[...] = jnp.where(ids == far_ref[...], 1.0, 0.0).astype(BF)
    loads["x"].wait()
    x = xe[pl.ds(GOT, NODE), :]
    near_src[...] = t_dot(own_near[...], x).astype(BF).reshape(6, 16, D)
    far_src[...] = t_dot(own_far[...], x).astype(BF).reshape(FAR, 4, 128)

    pl.semaphore_wait(barrier, 66)

    nears = []
    for k, o in enumerate(OFFSETS):
        one = pltpu.make_async_remote_copy(
            src_ref=near_src.at[k], dst_ref=near_got.at[k],
            send_sem=near_send.at[k], recv_sem=near_recv.at[k],
            device_id=patch_id((me + o + 64) % 64), device_id_type=MESH,
        )
        one.start()
        nears.append(one)

    def remote(src, dst, sems, k, device):
        one = pltpu.make_async_remote_copy(
            src_ref=src, dst_ref=dst, send_sem=sems[0].at[k], recv_sem=sems[1].at[k],
            device_id=device, device_id_type=MESH,
        )
        one.start()
        return one

    def plane(k):
        return {"patch_0": k // 2, "patch_2": k % 2}

    @pl.loop(0, 63, unroll=7)
    def _(k):
        to = (me + 1 + (k + 32) % 63) % 64
        pltpu.make_async_remote_copy(
            src_ref=far_src.at[to], dst_ref=far_got.at[me],
            send_sem=far_send.at[0], recv_sem=far_recv.at[0],
            device_id=patch_id(to), device_id_type=MESH,
        ).start()

    far_all = pltpu.make_async_remote_copy(
        src_ref=far_src.at[pl.ds(0, 63)], dst_ref=far_got.at[pl.ds(0, 63)],
        send_sem=far_send.at[0], recv_sem=far_recv.at[0],
        device_id=patch_id((me + 1) % 64), device_id_type=MESH,
    )

    spot = lax.broadcasted_iota(jnp.int32, (1, EDGE), 1)
    live = spot < count_ref[0]
    loads["sender"].wait()
    loads["receiver"].wait()
    s_row = sender_ref[...].reshape(1, EDGE)
    s_row = jnp.where(live, jnp.where(s_row < NODE, s_row + GOT, s_row - NODE), -1)
    r_row = jnp.where(live, receiver_ref[...].reshape(1, EDGE) + EXT, -1)
    cols = columns([s_row.astype(F32), r_row.astype(F32)])
    s_col = cols[:, 0:1].astype(jnp.int32)
    r_col = cols[:, 1:2].astype(jnp.int32)
    for k in range(TABLE // 128):
        ids = lax.broadcasted_iota(jnp.int32, (EDGE, 128), 1) + k * 128
        which = s_col if k < EXT // 128 else r_col
        onehot[:, pl.ds(k * 128, 128)] = jnp.where(ids == which, 1.0, 0.0).astype(BF)
    for k in range(TABLE // 128):
        ids = lax.broadcasted_iota(jnp.int32, (128, EDGE), 0) + k * 128
        which = s_row if k < EXT // 128 else r_row
        onehot_t[pl.ds(k * 128, 128), :] = jnp.where(ids == which, 1.0, 0.0).astype(BF)

    loads["we_in"].wait()
    proj[pl.ds(GOT, NODE), :] = dot(x, we_in[pl.ds(0, D), :]).astype(BF)
    proj[pl.ds(EXT, NODE), :] = dot(x, we_in[pl.ds(D, D), :]).astype(BF)
    loads["e"].wait()
    pre[...] = dot(e[...], we_in[pl.ds(2 * D, D), :]) + dot(
        onehot[:, pl.ds(GOT, 2 * NODE)], proj[pl.ds(GOT, 2 * NODE), :]
    )

    for one in nears:
        one.wait_recv()
    far_all.wait_recv()
    xe[pl.ds(0, NEAR), :] = near_got[...].reshape(NEAR, D)
    slot = lax.broadcasted_iota(jnp.int32, (FAR, 4, 128), 0)
    far_rows = jnp.where(slot == me, far_src[...], far_got[...]).reshape(FAR, D)
    xe[pl.ds(NEAR, FAR), :] = far_rows
    xe[pl.ds(NEAR + FAR, 96), :] = jnp.zeros((96, D), BF)
    proj[pl.ds(0, GOT), :] = dot(xe[pl.ds(0, GOT), :], we_in[pl.ds(0, D), :]).astype(BF)

    loads["we_out"].wait()

    for k in range(EDGE // TILE):
        at = pl.ds(k * TILE, TILE)
        v = pre[at, :] + dot(onehot[at, pl.ds(0, GOT)], proj[pl.ds(0, GOT), :])
        s = jax.nn.sigmoid(v)
        h = (v * s).astype(BF)
        hid[at, :] = h
        pre[at, :] = s * (1.0 + v * (1.0 - s))
        normed, inverse = normalize(dot(h, we_out[...]))
        msg[at, :] = normed.astype(BF)
        inv[at, :] = jnp.broadcast_to(inverse, (TILE, 128))

    aggregate = dot(onehot_t[pl.ds(EXT, NODE), :], msg[...]).astype(BF)

    loads["wn_in"].wait()
    node_pre = dot(x, wn_in[pl.ds(0, D), :]) + dot(aggregate, wn_in[pl.ds(D, D), :])
    s = jax.nn.sigmoid(node_pre)
    node_hidden = (node_pre * s).astype(BF)
    node_slope = s * (1.0 + node_pre * (1.0 - s))
    loads["wn_out"].wait()
    node_normed, node_inverse = normalize(dot(node_hidden, wn_out[...]))
    updated = (x.astype(F32) + node_normed).astype(BF)
    loads["wr"].wait()
    predicted = dot(updated, wr[...])
    loads["land"].wait()
    loads["lat"].wait()
    latitude = -0.5 * jnp.pi + (lat_ref[...].reshape(1, NODE).astype(F32) + 0.5) * (jnp.pi / BANDS)
    cols = columns([jnp.cos(latitude), land_ref[...].reshape(1, NODE).astype(F32)])
    area, land = cols[:, 0:1], cols[:, 1:2]
    channel = lax.broadcasted_iota(jnp.int32, (NODE, 128), 1)
    weight = jnp.where((channel < OCEAN) & (land == 1.0), 0.0, area)
    loads["t"].wait()
    pred_grad = (weight * (predicted - tgt[...].astype(F32))).astype(BF)
    updated_grad = dot_t(pred_grad, wr[...])
    node_z_grad = norm_back(updated_grad, node_normed, node_inverse).astype(BF)
    node_pre_grad = (dot_t(node_z_grad, wn_out[...]) * node_slope).astype(BF)
    total[...] = updated_grad + dot_t(node_pre_grad, wn_in[pl.ds(0, D), :])
    agg_grad[...] = dot_t(node_pre_grad, wn_in[pl.ds(D, D), :]).astype(BF)

    where = (ix, iy, iz, ic)
    ga, gb = Reducer(group_a, where), Reducer(group_b, where)

    def pack_rows(start0, value, blocks, slots):
        rows = value.reshape(4, 8, 2, blocks, 8, D)
        for b, (h, t) in enumerate(slots):
            for c in range(2):
                for y in range(4):
                    tile = rows[:, :, c, b, :, y * 128 : (y + 1) * 128].astype(BF)
                    if h == 0:
                        start0[h, c, :, y, :, t] = tile
                    else:
                        start0[h, c, y, :, :, t] = tile

    wgrad[pl.ds(0, D), :] = t_dot(x, node_pre_grad)
    wgrad[pl.ds(D, D), :] = t_dot(aggregate, node_pre_grad)
    pack_rows(ga.start0, wgrad[pl.ds(0, 2 * D), :], 2, ((0, 0), (0, 1)))
    pack_rows(ga.start0, t_dot(node_hidden, node_z_grad), 1, ((1, 0),))
    readout = t_dot(updated, pred_grad).reshape(4, 8, 2, 8, 128)
    for c in range(2):
        for y in range(4):
            ga.start0[1, c, y, :, :, 1] = readout[:, :, c].astype(BF)
    ga.pair()

    def edge_backward(k):
        at = pl.ds(k * TILE, TILE)
        g = dot(onehot[at, pl.ds(EXT, NODE)], agg_grad[...])
        z_grad = norm_back(g, msg[at, :].astype(F32), inv[at, :][:, 0:1]).astype(BF)
        ezg[at, :] = z_grad
        epg[at, :] = (dot_t(z_grad, we_out[...]) * pre[at, :]).astype(BF)

    for k in range(EDGE // TILE):
        edge_backward(k)
        if k == 2:
            ga.first()
    gsum[...] = dot(onehot_t[...], epg[...]).astype(BF)
    ga.middle()

    wgrad[pl.ds(0, D), :] = t_dot(xe[...], gsum[pl.ds(0, EXT), :])
    wgrad[pl.ds(D, D), :] = t_dot(x, gsum[pl.ds(EXT, NODE), :])
    wgrad[pl.ds(2 * D, D), :] = t_dot(e[...], epg[...])
    pack_rows(gb.start0, wgrad[...], 3, ((0, 0), (0, 1), (1, 0)))
    pack_rows(gb.start0, t_dot(hid[...], ezg[...]), 1, ((1, 1),))
    gb.pair()
    back = dot_t(gsum[pl.ds(0, GOT), :], we_in[pl.ds(0, D), :])
    back_near_src[...] = back[0:NEAR].astype(BF).reshape(6, 16, D)
    back_far_src[...] = back[NEAR : NEAR + FAR].astype(BF).reshape(4, 8, 2, 4, 128)
    backs = []
    for k, o in enumerate(OFFSETS):
        one = pltpu.make_async_remote_copy(
            src_ref=back_near_src.at[k], dst_ref=back_near_got.at[k],
            send_sem=bnear_send.at[k], recv_sem=bnear_recv.at[k],
            device_id=patch_id((me - o + 64) % 64), device_id_type=MESH,
        )
        one.start()
        backs.append(one)

    spot_xc = ix * 2 + ic
    bfars = []

    def remote(src, dst, sems, k, device):
        one = pltpu.make_async_remote_copy(
            src_ref=src, dst_ref=dst, send_sem=sems[0].at[k], recv_sem=sems[1].at[k],
            device_id=device, device_id_type=MESH,
        )
        one.start()
        return one

    for d in range(1, 8):
        to = (iz + d) % 8
        bfars.append(remote(
            back_far_src.at[:, to], back_far_mid.at[iz], (bfar_send, bfar_recv), d - 1,
            {"patch_1": to},
        ))
    back_far_mid[pl.ds(iz, 1)] = back_far_src[:, pl.ds(iz, 1)].reshape(1, 4, 2, 4, 128)

    edge_res[...] = dot_t(epg[...], we_in[pl.ds(2 * D, D), :]).astype(BF)
    edge_copy = pltpu.make_async_copy(edge_res, edge_out.at[0], out_sem.at[0])
    edge_copy.start()
    gb.first()
    ga.second()
    total[...] += dot_t(gsum[pl.ds(GOT, NODE), :], we_in[pl.ds(0, D), :]) + dot_t(
        gsum[pl.ds(EXT, NODE), :], we_in[pl.ds(D, D), :]
    )
    gb.middle()

    for one in bfars:
        one.wait_recv()
    for d in range(1, 8):
        to = (spot_xc + d) % 8
        bfars.append(remote(
            back_far_mid.at[:, to // 2, to % 2], back_far_got.at[ix, :, ic],
            (bfar_send, bfar_recv), 6 + d, {"patch_0": to // 2, "patch_2": to % 2},
        ))
    back_far_got[pl.ds(ix, 1), :, pl.ds(ic, 1)] = back_far_mid[
        :, pl.ds(ix, 1), pl.ds(ic, 1)
    ].reshape(1, 8, 1, 4, 128)
    gb.second()
    ga.third()

    for one in backs + bfars[7:]:
        one.wait_recv()
    far_rows = back_far_got[...].reshape(FAR, D)
    owned = dot(own_near[...], back_near_got[...].reshape(NEAR, D)) + dot(own_far[...], far_rows)
    node_res[...] = (total[...] + owned).astype(BF)
    node_copy = pltpu.make_async_copy(node_res, node_out.at[0], out_sem.at[1])
    node_copy.start()

    gb.third()
    ga.fourth()
    gb.fourth()
    parts = ga.last()
    for y in range(4):
        at = pl.ds(y * 128, 128)
        grads[pl.ds(32, 8), at] = parts[y][0, 0]
        grads[pl.ds(40, 8), at] = parts[y][0, 1]
        grads[pl.ds(48, 8), at] = parts[y][1, 0]
    grads[pl.ds(56, 8), pl.ds(0, 128)] = parts[0][1, 1]
    grads[pl.ds(56, 8), pl.ds(128, 384)] = jnp.zeros((8, 384), F32)
    parts = gb.last()
    for y in range(4):
        at = pl.ds(y * 128, 128)
        grads[pl.ds(0, 8), at] = parts[y][0, 0]
        grads[pl.ds(8, 8), at] = parts[y][0, 1]
        grads[pl.ds(16, 8), at] = parts[y][1, 0]
        grads[pl.ds(24, 8), at] = parts[y][1, 1]
    grads_copy = pltpu.make_async_copy(grads, grads_out, dma_sem.at[0])
    grads_copy.start()

    grads_copy.wait()
    node_copy.wait()
    edge_copy.wait()
    for one in nears + backs + bfars:
        one.wait_send()
    far_all.wait_send()
    ga.finish()
    gb.finish()


def hand_out(node, edge, grads, *rest):
    outs, (node_v, edge_v, grads_v, take_sem, give_sem) = rest[:7], rest[7:]
    parts = ((0, 24, D), (24, 8, D), (32, 16, D), (48, 8, D), (56, 8, 128))
    steps = [(grads, grads_v, [
        (grads_v.at[pl.ds(at, n), pl.ds(0, w)], outs[2 + k]) for k, (at, n, w) in enumerate(parts)
    ])]
    for k in range(5):
        at = pl.ds(k * TILE, TILE)
        steps.append((edge.at[0, at], edge_v.at[at], [(edge_v.at[at], outs[1].at[0, at])]))
    steps.append((node.at[0], node_v, [(node_v, outs[0].at[0])]))
    takes, gives = [], []
    for k, (src, dst, _) in enumerate(steps):
        takes.append(pltpu.make_async_copy(src, dst, take_sem.at[k]))
        takes[-1].start()
    for k, (_, _, moves) in enumerate(steps):
        takes[k].wait()
        for src, dst in moves:
            gives.append(pltpu.make_async_copy(src, dst, give_sem.at[len(gives)]))
            gives[-1].start()
    for one in gives:
        one.wait()


def group_scratch():
    tail = (8, 128)
    return [
        pltpu.VMEM((2, 2, 4, 4, 8, 2, *tail), BF),
        pltpu.VMEM((2, 4, 4, 8, 2, *tail), BF),
        pltpu.VMEM((2, 4, 4, 8, 2, *tail), BF),
        pltpu.VMEM((2, 2, 2, 8, 2, *tail), BF),
        pltpu.VMEM((2, 2, 2, 8, 2, *tail), BF),
        pltpu.VMEM((2, 2, 2, 8, 2, *tail), BF),
        pltpu.VMEM((2, 2, 2, 8, 2, *tail), BF),
        pltpu.VMEM((2, 4, 8, 2, *tail), BF),
        pltpu.VMEM((2, 3, 8, 2, *tail), BF),
        pltpu.VMEM((8, 2, 2, *tail), BF),
        pltpu.VMEM((7, 2, 2, *tail), BF),
        pltpu.VMEM((2, 2, *tail), F32),
        pltpu.VMEM((3, 2, 2, *tail), F32),
        pltpu.SemaphoreType.DMA((30,)),
        pltpu.SemaphoreType.DMA((30,)),
    ]


def body(*args):
    (x, e, t, we_in, we_out, wn_in, wn_out, wr, send, far, sender, receiver, count, land, lat) = args
    anywhere = pl.BlockSpec(memory_space=pl.ANY)
    hbm = pl.BlockSpec(memory_space=pltpu.HBM)
    near = pltpu.VMEM((6, 16, D), BF)
    row = pltpu.VMEM((FAR, 4, 128), BF)
    natural = pltpu.VMEM((4, 8, 2, 4, 128), BF)
    turned = pltpu.VMEM((8, 4, 2, 4, 128), BF)
    sem = pltpu.SemaphoreType.DMA
    scratch = [
        pltpu.VMEM((1, NEAR), jnp.int32),
        pltpu.VMEM((1, FAR), jnp.int32),
        pltpu.VMEM((EDGE,), jnp.int32),
        pltpu.VMEM((EDGE,), jnp.int32),
        pltpu.VMEM((NODE,), jnp.int32),
        pltpu.VMEM((NODE,), jnp.int32),
        pltpu.VMEM((EXT, D), BF),
        pltpu.VMEM((EDGE, D), BF),
        pltpu.VMEM((NODE, 128), BF),
        pltpu.VMEM((3 * D, D), BF),
        pltpu.VMEM((D, D), BF),
        pltpu.VMEM((2 * D, D), BF),
        pltpu.VMEM((D, D), BF),
        pltpu.VMEM((D, 128), BF),
        pltpu.VMEM((EDGE, D), BF),
        near, near, row, row, near, near, natural, turned, natural,
        pltpu.VMEM((EDGE, TABLE), BF),
        pltpu.VMEM((TABLE, EDGE), BF),
        pltpu.VMEM((NODE, NEAR), BF),
        pltpu.VMEM((NODE, FAR), BF),
        pltpu.VMEM((TABLE, D), BF),
        pltpu.VMEM((EDGE, D), F32),
        pltpu.VMEM((EDGE, D), BF),
        pltpu.VMEM((EDGE, D), BF),
        pltpu.VMEM((EDGE, 128), F32),
        pltpu.VMEM((EDGE, D), BF),
        pltpu.VMEM((EDGE, D), BF),
        pltpu.VMEM((NODE, D), F32),
        pltpu.VMEM((NODE, D), BF),
        pltpu.VMEM((TABLE, D), BF),
        pltpu.VMEM((3 * D, D), F32),
        pltpu.VMEM((NODE, D), BF),
        pltpu.VMEM((64, D), F32),
        sem((14,)), sem((2,)),
        sem((6,)), sem((6,)), sem((1,)), sem((1,)),
        sem((6,)), sem((6,)), sem((14,)), sem((14,)),
    ] + group_scratch() + group_scratch()
    shapes = (
        jax.ShapeDtypeStruct((1, NODE, D), BF),
        jax.ShapeDtypeStruct((1, EDGE, D), BF),
        jax.ShapeDtypeStruct((24, D), F32),
        jax.ShapeDtypeStruct((8, D), F32),
        jax.ShapeDtypeStruct((16, D), F32),
        jax.ShapeDtypeStruct((8, D), F32),
        jax.ShapeDtypeStruct((8, 128), F32),
    )
    results = pl.pallas_call(
        kernel,
        out_shape=(*shapes[:2], jax.ShapeDtypeStruct((64, D), F32)),
        in_specs=[hbm] * 12 + [pl.BlockSpec(memory_space=pltpu.SMEM)] + [hbm] * 2,
        out_specs=(anywhere,) * 3,
        scratch_shapes=scratch,
        compiler_params=pltpu.CompilerParams(
            collective_id=0, has_side_effects=True, vmem_limit_bytes=62 * 1024 * 1024
        ),
    )(
        x, e, t, we_in, we_out, wn_in, wn_out, wr, send, far,
        sender, receiver, count, land, lat,
    )
    return pl.pallas_call(
        hand_out,
        out_shape=shapes,
        in_specs=[anywhere] * 3,
        out_specs=(hbm,) * 7,
        scratch_shapes=[
            pltpu.VMEM((NODE, D), BF),
            pltpu.VMEM((EDGE, D), BF),
            pltpu.VMEM((64, D), F32),
            sem((7,)),
            sem((11,)),
        ],
        compiler_params=pltpu.CompilerParams(vmem_limit_bytes=60 * 1024 * 1024),
    )(*results)


def solution(mesh):
    split = Mesh(
        mesh.devices.reshape(4, 8, 2, mesh.shape["rep"]), ("patch_0", "patch_1", "patch_2", "rep")
    )
    in_specs = (
        P("rep", PATCH, None),
        P("rep", PATCH, None),
        P("rep", PATCH, None),
        P(),
        P(),
        P(),
        P(),
        P(),
        P(PATCH, None),
        P(PATCH, None),
        P(PATCH),
        P(PATCH),
        P(PATCH),
        P(PATCH),
        P(PATCH),
    )
    out_specs = (
        P("rep", PATCH, None),
        P("rep", PATCH, None),
        P(PATCH, None),
        P(PATCH, None),
        P(PATCH, None),
        P(PATCH, None),
        P(PATCH, None),
    )
    return jax.shard_map(body, mesh=split, in_specs=in_specs, out_specs=out_specs, check_vma=False)
```

```python
import functools

import jax
import jax.numpy as jnp
from jax import lax
from jax.experimental import pallas as pl
from jax.experimental.pallas import tpu as pltpu
from jax.sharding import Mesh
from jax.sharding import PartitionSpec as P

OCEAN = 32
BANDS = 721
PATCH = ("patch_0", "patch_1", "patch_2")
MESH = pl.DeviceIdType.MESH
D = 512
NODE = 384
EDGE = 1280
NEAR = 96
FAR = 64
EXT = 640
GOT = EXT - NODE
TABLE = EXT + NODE
TILE = 256
OFFSETS = (1, -1, 2, -2, 3, -3)
BF = jnp.bfloat16
F32 = jnp.float32


def dot(a, b):
    return jnp.dot(a, b, preferred_element_type=F32)


def dot_t(a, b):
    return lax.dot_general(a, b, (((1,), (1,)), ((), ())), preferred_element_type=F32)


def t_dot(a, b):
    return lax.dot_general(a, b, (((0,), (0,)), ((), ())), preferred_element_type=F32)


def patch_id(q):
    return {"patch_0": q // 16, "patch_1": (q // 2) % 8, "patch_2": q % 2}


def greet(barrier, device):
    pl.semaphore_signal(barrier, inc=1, device_id=device, device_id_type=MESH)


def normalize(v):
    mean = jnp.mean(v, axis=-1, keepdims=True)
    centred = v - mean
    var = jnp.mean(centred * centred, axis=-1, keepdims=True)
    inverse = lax.rsqrt(var + 1e-05)
    return centred * inverse, inverse


def norm_back(g, y, inverse):
    first = jnp.mean(g, axis=-1, keepdims=True)
    second = jnp.mean(g * y, axis=-1, keepdims=True)
    return inverse * (g - first - y * second)


def columns(rows):
    wide = rows[0].shape[1]
    pad = [jnp.zeros((8 - len(rows), wide), F32)]
    return jnp.concatenate(rows + pad, axis=0).T


class Reducer:
    def __init__(self, refs, where):
        (self.start0, self.r0, self.w1, self.direct, self.relay, self.merged, self.carried,
         self.w2, self.r2, self.w3, self.r3, self.w4, self.r4, self.send, self.recv) = refs
        x, self.y, self.z, self.c = where
        self.axes = ((("patch_0", x), ("rep", self.y)), (("rep", self.y), ("patch_0", x)))
        self.pending = []

    def copy(self, src, dst, k, device):
        one = pltpu.make_async_remote_copy(
            src_ref=src, dst_ref=dst, send_sem=self.send.at[k], recv_sem=self.recv.at[k],
            device_id=device, device_id_type=MESH,
        )
        one.start()
        self.pending.append(one)
        return one

    def pair(self):
        other = 1 - self.c
        self.c0 = [
            self.copy(self.start0.at[h, other], self.r0.at[h], h, {"patch_2": other})
            for h in range(2)
        ]

    def first(self):
        self.c1 = []
        for h in range(2):
            self.c0[h].wait_recv()

            @pl.loop(0, 4)
            def _(i):
                mine = self.start0[h, self.c, i].astype(F32)
                self.w1[h, i] = (mine + self.r0[h, i].astype(F32)).astype(BF)

            axis, at = self.axes[h][0]
            right, left, across = (at + 1) % 4, (at + 3) % 4, (at + 2) % 4
            lo, hi = pl.ds(0, 2), pl.ds(2, 2)
            w1, k = self.w1, 2 + 6 * h
            self.c1.append((
                self.copy(w1.at[h, across, lo], self.relay.at[h, 0], k, {axis: right}),
                self.copy(w1.at[h, across, hi], self.relay.at[h, 1], k + 1, {axis: left}),
                self.copy(w1.at[h, left, lo], self.direct.at[h, 0], k + 2, {axis: left}),
                self.copy(w1.at[h, right, hi], self.direct.at[h, 1], k + 3, {axis: right}),
            ))

    def middle(self):
        self.c1b = []
        for h in range(2):
            axis, at = self.axes[h][0]
            ends = ((at + 1) % 4, (at + 3) % 4)
            for side in range(2):
                self.c1[h][side].wait_recv()
                mine = self.w1[h, ends[side], pl.ds(2 * side, 2)].astype(F32)
                self.merged[h, side] = (mine + self.relay[h, side].astype(F32)).astype(BF)
                self.c1b.append(self.copy(
                    self.merged.at[h, side], self.carried.at[h, side], 6 + 6 * h + side,
                    {axis: ends[side]},
                ))

    def second(self):
        self.c2 = []
        for h in range(2):
            _, own = self.axes[h][0]
            for side in range(2):
                self.c1[h][2 + side].wait_recv()
                self.c1b[2 * h + side].wait_recv()
                part = pl.ds(2 * side, 2)
                acc = self.w1[h, own, part].astype(F32) + self.direct[h, side].astype(F32)
                self.w2[h, part] = (acc + self.carried[h, side].astype(F32)).astype(BF)
            axis, at = self.axes[h][1]
            for d in range(1, 4):
                to = (at + d) % 4
                self.c2.append(
                    self.copy(self.w2.at[h, to], self.r2.at[h, d - 1], 13 + 3 * h + d, {axis: to})
                )

    def third(self):
        for h in range(2):
            for one in self.c2[3 * h : 3 * h + 3]:
                one.wait_recv()
            acc = self.w2[h, self.axes[h][1][1]].astype(F32)
            for s in range(3):
                acc = acc + self.r2[h, s].astype(F32)
            self.w3[:, h] = acc.astype(BF)
        self.c3 = []
        for d in range(1, 8):
            to = (self.z + d) % 8
            self.c3.append(self.copy(self.w3.at[to], self.r3.at[d - 1], 19 + d, {"patch_1": to}))

    def fourth(self):
        for one in self.c3:
            one.wait_recv()
        acc = self.w3[self.z].astype(F32)
        for s in range(7):
            acc = acc + self.r3[s].astype(F32)
        self.w4[...] = acc * (1.0 / (NODE * 64 * 4))
        self.c4 = []
        for d in range(1, 4):
            to = (self.y + d) % 4
            self.c4.append(self.copy(self.w4, self.r4.at[d - 1], 26 + d, {"rep": to}))

    def last(self):
        for one in self.c4:
            one.wait_recv()
        out = []
        own = self.w4[...]
        got = [self.r4[s] for s in range(3)]
        for y in range(4):
            tile = own
            for s in range(3):
                tile = jnp.where((self.y - s - 1 + 4) % 4 == y, got[s], tile)
            out.append(tile)
        return out

    def finish(self):
        for one in self.pending:
            one.wait_send()


def kernel(
    x_hbm, e_hbm, t_hbm, we_in_hbm, we_out_hbm, wn_in_hbm, wn_out_hbm, wr_hbm,
    send_hbm, far_hbm, sender_hbm, receiver_hbm, count_ref, land_hbm, lat_hbm,
    node_out, edge_out, grads_out,
    send_ref, far_ref, sender_ref, receiver_ref, land_ref, lat_ref,
    xe, e, tgt, we_in, we_out, wn_in, wn_out, wr,
    near_src, near_got, far_src, far_got, back_near_src, back_near_got, back_far_src, back_far_mid, back_far_got,
    onehot, onehot_t, own_near, own_far, proj, pre, hid, msg, inv, ezg, epg, total, agg_grad, gsum, wgrad,
    *rest,
):
    dma_sem, near_send, near_recv, far_send, far_recv = rest[:5]
    bnear_send, bnear_recv, bfar_send, bfar_recv = rest[5:9]
    group_a, group_b = rest[9:24], rest[24:39]
    ix, iz, ic, iy = (lax.axis_index(a) for a in (*PATCH, "rep"))
    me = ix * 16 + iz * 2 + ic

    loads = {}
    for k, (name, src, dst) in enumerate((
        ("send", send_hbm, send_ref),
        ("far", far_hbm, far_ref),
        ("sender", sender_hbm, sender_ref),
        ("receiver", receiver_hbm, receiver_ref),
        ("x", x_hbm.at[0], xe.at[pl.ds(GOT, NODE)]),
        ("we_in", we_in_hbm, we_in),
        ("e", e_hbm.at[0], e),
        ("we_out", we_out_hbm, we_out),
        ("wn_in", wn_in_hbm, wn_in),
        ("wn_out", wn_out_hbm, wn_out),
        ("wr", wr_hbm, wr),
        ("t", t_hbm.at[0], tgt),
        ("land", land_hbm, land_ref),
        ("lat", lat_hbm, lat_ref),
    )):
        loads[name] = pltpu.make_async_copy(src, dst, dma_sem.at[k])
        loads[name].start()

    barrier = pltpu.get_barrier_semaphore()

    xs, zs, cs = ([(i + d) % n for d in range(n)] for i, n in ((ix, 4), (iz, 8), (ic, 2)))
    others = [
        (dx, dz, dc)
        for dx in (2, 1, 3, 0)
        for dz in (4, 3, 5, 2, 6, 1, 7, 0)
        for dc in range(2)
        if dx or dz or dc
    ]
    for dx, dz, dc in others:
        greet(barrier, {"patch_0": xs[dx], "patch_1": zs[dz], "patch_2": cs[dc]})

    for d in range(1, 4):
        greet(barrier, {"rep": (iy + d) % 4})

    loads["send"].wait()
    loads["far"].wait()
    ids = lax.broadcasted_iota(jnp.int32, (NODE, NEAR), 0)
    own_near[...] = jnp.where(ids == send_ref[...], 1.0, 0.0).astype(BF)
    ids = lax.broadcasted_iota(jnp.int32, (NODE, FAR), 0)
    own_far[...] = jnp.where(ids == far_ref[...], 1.0, 0.0).astype(BF)
    loads["x"].wait()
    x = xe[pl.ds(GOT, NODE), :]
    near_src[...] = t_dot(own_near[...], x).astype(BF).reshape(6, 16, D)
    far_src[...] = t_dot(own_far[...], x).astype(BF).reshape(4, 8, 2, 4, 128)

    pl.semaphore_wait(barrier, 66)

    nears = []
    for k, o in enumerate(OFFSETS):
        one = pltpu.make_async_remote_copy(
            src_ref=near_src.at[k], dst_ref=near_got.at[k],
            send_sem=near_send.at[k], recv_sem=near_recv.at[k],
            device_id=patch_id((me + o + 64) % 64), device_id_type=MESH,
        )
        one.start()
        nears.append(one)

    def remote(src, dst, sems, k, device):
        one = pltpu.make_async_remote_copy(
            src_ref=src, dst_ref=dst, send_sem=sems[0].at[k], recv_sem=sems[1].at[k],
            device_id=device, device_id_type=MESH,
        )
        one.start()
        return one

    def plane(k):
        return {"patch_0": k // 2, "patch_2": k % 2}

    for dx, dz, dc in others:
        pltpu.make_async_remote_copy(
            src_ref=far_src.at[xs[dx], zs[dz], cs[dc]], dst_ref=far_got.at[me],
            send_sem=far_send.at[0], recv_sem=far_recv.at[0],
            device_id={"patch_0": xs[dx], "patch_1": zs[dz], "patch_2": cs[dc]},
            device_id_type=MESH,
        ).start()

    far_all = pltpu.make_async_remote_copy(
        src_ref=far_got.at[pl.ds(0, 63)], dst_ref=far_got.at[pl.ds(0, 63)],
        send_sem=far_send.at[0], recv_sem=far_recv.at[0],
        device_id=patch_id((me + 1) % 64), device_id_type=MESH,
    )

    spot = lax.broadcasted_iota(jnp.int32, (1, EDGE), 1)
    live = spot < count_ref[0]
    loads["sender"].wait()
    loads["receiver"].wait()
    s_row = sender_ref[...].reshape(1, EDGE)
    s_row = jnp.where(live, jnp.where(s_row < NODE, s_row + GOT, s_row - NODE), -1)
    r_row = jnp.where(live, receiver_ref[...].reshape(1, EDGE) + EXT, -1)
    cols = columns([s_row.astype(F32), r_row.astype(F32)])
    s_col = cols[:, 0:1].astype(jnp.int32)
    r_col = cols[:, 1:2].astype(jnp.int32)
    for k in range(TABLE // 128):
        ids = lax.broadcasted_iota(jnp.int32, (EDGE, 128), 1) + k * 128
        which = s_col if k < EXT // 128 else r_col
        onehot[:, pl.ds(k * 128, 128)] = jnp.where(ids == which, 1.0, 0.0).astype(BF)
    for k in range(TABLE // 128):
        ids = lax.broadcasted_iota(jnp.int32, (128, EDGE), 0) + k * 128
        which = s_row if k < EXT // 128 else r_row
        onehot_t[pl.ds(k * 128, 128), :] = jnp.where(ids == which, 1.0, 0.0).astype(BF)

    loads["we_in"].wait()
    proj[pl.ds(GOT, NODE), :] = dot(x, we_in[pl.ds(0, D), :]).astype(BF)
    proj[pl.ds(EXT, NODE), :] = dot(x, we_in[pl.ds(D, D), :]).astype(BF)
    loads["e"].wait()
    pre[...] = dot(e[...], we_in[pl.ds(2 * D, D), :]) + dot(
        onehot[:, pl.ds(GOT, 2 * NODE)], proj[pl.ds(GOT, 2 * NODE), :]
    )

    loads["wn_in"].wait()
    total[...] = dot(x, wn_in[pl.ds(0, D), :])
    for one in nears:
        one.wait_recv()
    far_all.wait_recv()
    xe[pl.ds(0, NEAR), :] = near_got[...].reshape(NEAR, D)
    slot = lax.broadcasted_iota(jnp.int32, (FAR, 4, 128), 0)
    far_rows = jnp.where(slot == me, far_src[...].reshape(FAR, 4, 128), far_got[...]).reshape(FAR, D)
    xe[pl.ds(NEAR, FAR), :] = far_rows
    xe[pl.ds(NEAR + FAR, 96), :] = jnp.zeros((96, D), BF)
    proj[pl.ds(0, GOT), :] = dot(xe[pl.ds(0, GOT), :], we_in[pl.ds(0, D), :]).astype(BF)

    loads["we_out"].wait()

    count = EDGE // TILE
    tiles = [pl.ds(k * TILE, TILE) for k in range(count)]

    def enter(k):
        return pre[tiles[k], :] + dot(onehot[tiles[k], pl.ds(0, GOT)], proj[pl.ds(0, GOT), :])

    def activate(k, v):
        s = jax.nn.sigmoid(v)
        h = (v * s).astype(BF)
        hid[tiles[k], :] = h
        pre[tiles[k], :] = s * (1.0 + v * (1.0 - s))
        return dot(h, we_out[...])

    def settle(k, out):
        normed, inverse = normalize(out)
        msg[tiles[k], :] = normed.astype(BF)
        inv[tiles[k], :] = jnp.broadcast_to(inverse, (TILE, 128))

    v, out = enter(0), None
    for k in range(count):
        v_next = enter(k + 1) if k + 1 < count else None
        out_next = activate(k, v)
        if out is not None:
            settle(k - 1, out)
        v, out = v_next, out_next
    settle(count - 1, out)

    aggregate = dot(onehot_t[pl.ds(EXT, NODE), :], msg[...]).astype(BF)

    node_pre = total[...] + dot(aggregate, wn_in[pl.ds(D, D), :])
    s = jax.nn.sigmoid(node_pre)
    node_hidden = (node_pre * s).astype(BF)
    node_slope = s * (1.0 + node_pre * (1.0 - s))
    loads["wn_out"].wait()
    node_normed, node_inverse = normalize(dot(node_hidden, wn_out[...]))
    updated = (x.astype(F32) + node_normed).astype(BF)
    loads["wr"].wait()
    predicted = dot(updated, wr[...])
    loads["land"].wait()
    loads["lat"].wait()
    latitude = -0.5 * jnp.pi + (lat_ref[...].reshape(1, NODE).astype(F32) + 0.5) * (jnp.pi / BANDS)
    cols = columns([jnp.cos(latitude), land_ref[...].reshape(1, NODE).astype(F32)])
    area, land = cols[:, 0:1], cols[:, 1:2]
    channel = lax.broadcasted_iota(jnp.int32, (NODE, 128), 1)
    weight = jnp.where((channel < OCEAN) & (land == 1.0), 0.0, area)
    loads["t"].wait()
    pred_grad = (weight * (predicted - tgt[...].astype(F32))).astype(BF)
    updated_grad = dot_t(pred_grad, wr[...])
    node_z_grad = norm_back(updated_grad, node_normed, node_inverse).astype(BF)
    node_pre_grad = (dot_t(node_z_grad, wn_out[...]) * node_slope).astype(BF)
    total[...] = updated_grad + dot_t(node_pre_grad, wn_in[pl.ds(0, D), :])
    aggregate_grad = dot_t(node_pre_grad, wn_in[pl.ds(D, D), :])
    centre = jnp.mean(aggregate_grad, axis=-1, keepdims=True)
    agg_grad[...] = (aggregate_grad - centre).astype(BF)

    where = (ix, iy, iz, ic)
    ga, gb = Reducer(group_a, where), Reducer(group_b, where)

    def pack_rows(start0, value, blocks, slots):
        rows = value.reshape(4, 8, 2, blocks, 8, D)
        for b, (h, t) in enumerate(slots):
            for c in range(2):
                for y in range(4):
                    tile = rows[:, :, c, b, :, y * 128 : (y + 1) * 128].astype(BF)
                    if h == 0:
                        start0[h, c, :, y, :, t] = tile
                    else:
                        start0[h, c, y, :, :, t] = tile

    wgrad[pl.ds(0, D), :] = t_dot(x, node_pre_grad)
    wgrad[pl.ds(D, D), :] = t_dot(aggregate, node_pre_grad)
    pack_rows(ga.start0, wgrad[pl.ds(0, 2 * D), :], 2, ((0, 0), (0, 1)))
    pack_rows(ga.start0, t_dot(node_hidden, node_z_grad), 1, ((1, 0),))
    readout = t_dot(updated, pred_grad).reshape(4, 8, 2, 8, 128)
    for c in range(2):
        for y in range(4):
            ga.start0[1, c, y, :, :, 1] = readout[:, :, c].astype(BF)
    ga.pair()

    def gather(k):
        return dot(onehot[tiles[k], pl.ds(EXT, NODE)], agg_grad[...])

    def norm_step(k, g):
        y = msg[tiles[k], :].astype(F32)
        second = jnp.mean(g * y, axis=-1, keepdims=True)
        z_grad = (inv[tiles[k], :][:, 0:1] * (g - y * second)).astype(BF)
        ezg[tiles[k], :] = z_grad
        return dot_t(z_grad, we_out[...])

    def slope_step(k, out):
        epg[tiles[k], :] = (out * pre[tiles[k], :]).astype(BF)

    g, out = gather(0), None
    for k in range(count):
        g_next = gather(k + 1) if k + 1 < count else None
        out_next = norm_step(k, g)
        if out is not None:
            slope_step(k - 1, out)
        g, out = g_next, out_next
        if k == 2:
            ga.first()
    slope_step(count - 1, out)

    gsum[...] = dot(onehot_t[...], epg[...]).astype(BF)

    wgrad[pl.ds(2 * D, D), :] = t_dot(e[...], epg[...])
    pack_rows(gb.start0, t_dot(hid[...], ezg[...]), 1, ((1, 1),))
    ga.middle()
    wgrad[pl.ds(0, D), :] = t_dot(xe[...], gsum[pl.ds(0, EXT), :])
    wgrad[pl.ds(D, D), :] = t_dot(x, gsum[pl.ds(EXT, NODE), :])
    pack_rows(gb.start0, wgrad[...], 3, ((0, 0), (0, 1), (1, 0)))
    gb.pair()
    back = dot_t(gsum[pl.ds(0, GOT), :], we_in[pl.ds(0, D), :])
    back_near_src[...] = back[0:NEAR].astype(BF).reshape(6, 16, D)
    back_far_src[...] = back[NEAR : NEAR + FAR].astype(BF).reshape(4, 8, 2, 4, 128)
    backs = []
    for k, o in enumerate(OFFSETS):
        one = pltpu.make_async_remote_copy(
            src_ref=back_near_src.at[k], dst_ref=back_near_got.at[k],
            send_sem=bnear_send.at[k], recv_sem=bnear_recv.at[k],
            device_id=patch_id((me - o + 64) % 64), device_id_type=MESH,
        )
        one.start()
        backs.append(one)

    spot_xc = ix * 2 + ic
    bfars = []

    def remote(src, dst, sems, k, device):
        one = pltpu.make_async_remote_copy(
            src_ref=src, dst_ref=dst, send_sem=sems[0].at[k], recv_sem=sems[1].at[k],
            device_id=device, device_id_type=MESH,
        )
        one.start()
        return one

    for d in range(1, 8):
        to = (iz + d) % 8
        bfars.append(remote(
            back_far_src.at[:, to], back_far_mid.at[iz], (bfar_send, bfar_recv), d - 1,
            {"patch_1": to},
        ))
    back_far_mid[pl.ds(iz, 1)] = back_far_src[:, pl.ds(iz, 1)].reshape(1, 4, 2, 4, 128)

    edge_out[0] = dot_t(epg[...], we_in[pl.ds(2 * D, D), :]).astype(BF)
    gb.first()
    ga.second()
    total[...] += dot_t(gsum[pl.ds(GOT, NODE), :], we_in[pl.ds(0, D), :]) + dot_t(
        gsum[pl.ds(EXT, NODE), :], we_in[pl.ds(D, D), :]
    )
    gb.middle()

    for one in bfars:
        one.wait_recv()
    for d in range(1, 8):
        to = (spot_xc + d) % 8
        bfars.append(remote(
            back_far_mid.at[:, to // 2, to % 2], back_far_got.at[ix, :, ic],
            (bfar_send, bfar_recv), 6 + d, {"patch_0": to // 2, "patch_2": to % 2},
        ))
    back_far_got[pl.ds(ix, 1), :, pl.ds(ic, 1)] = back_far_mid[
        :, pl.ds(ix, 1), pl.ds(ic, 1)
    ].reshape(1, 8, 1, 4, 128)
    gb.second()
    ga.third()

    for one in backs + bfars[7:]:
        one.wait_recv()
    far_rows = back_far_got[...].reshape(FAR, D)
    owned = dot(own_near[...], back_near_got[...].reshape(NEAR, D)) + dot(own_far[...], far_rows)
    node_out[0] = (total[...] + owned).astype(BF)

    gb.third()
    ga.fourth()
    gb.fourth()
    parts = ga.last()
    for y in range(4):
        at = pl.ds(y * 128, 128)
        grads_out[pl.ds(32, 8), at] = parts[y][0, 0]
        grads_out[pl.ds(40, 8), at] = parts[y][0, 1]
        grads_out[pl.ds(48, 8), at] = parts[y][1, 0]
    grads_out[pl.ds(56, 8), pl.ds(0, 128)] = parts[0][1, 1]
    grads_out[pl.ds(56, 8), pl.ds(128, 384)] = jnp.zeros((8, 384), F32)
    parts = gb.last()
    for y in range(4):
        at = pl.ds(y * 128, 128)
        grads_out[pl.ds(0, 8), at] = parts[y][0, 0]
        grads_out[pl.ds(8, 8), at] = parts[y][0, 1]
        grads_out[pl.ds(16, 8), at] = parts[y][1, 0]
        grads_out[pl.ds(24, 8), at] = parts[y][1, 1]

    for one in nears + backs + bfars:
        one.wait_send()
    far_all.wait_send()
    ga.finish()
    gb.finish()


def hand_out(node, edge, grads, *rest):
    outs, sems = rest[:7], rest[7]
    parts = ((0, 24, D), (24, 8, D), (32, 16, D), (48, 8, D), (56, 8, 128))
    moves = [(edge, outs[1]), (node, outs[0])] + [
        (grads.at[pl.ds(at, n), pl.ds(0, w)], outs[2 + k]) for k, (at, n, w) in enumerate(parts)
    ]
    gives = [pltpu.make_async_copy(src, dst, sems.at[k]) for k, (src, dst) in enumerate(moves)]
    for one in gives:
        one.start()
    for one in gives:
        one.wait()


def group_scratch():
    tail = (8, 128)
    return [
        pltpu.VMEM((2, 2, 4, 4, 8, 2, *tail), BF),
        pltpu.VMEM((2, 4, 4, 8, 2, *tail), BF),
        pltpu.VMEM((2, 4, 4, 8, 2, *tail), BF),
        pltpu.VMEM((2, 2, 2, 8, 2, *tail), BF),
        pltpu.VMEM((2, 2, 2, 8, 2, *tail), BF),
        pltpu.VMEM((2, 2, 2, 8, 2, *tail), BF),
        pltpu.VMEM((2, 2, 2, 8, 2, *tail), BF),
        pltpu.VMEM((2, 4, 8, 2, *tail), BF),
        pltpu.VMEM((2, 3, 8, 2, *tail), BF),
        pltpu.VMEM((8, 2, 2, *tail), BF),
        pltpu.VMEM((7, 2, 2, *tail), BF),
        pltpu.VMEM((2, 2, *tail), F32),
        pltpu.VMEM((3, 2, 2, *tail), F32),
        pltpu.SemaphoreType.DMA((30,)),
        pltpu.SemaphoreType.DMA((30,)),
    ]


def body(*args):
    (x, e, t, we_in, we_out, wn_in, wn_out, wr, send, far, sender, receiver, count, land, lat) = args
    hbm = pl.BlockSpec(memory_space=pltpu.HBM)
    vmem = pl.BlockSpec(memory_space=pltpu.VMEM)
    near = pltpu.VMEM((6, 16, D), BF)
    row = pltpu.VMEM((FAR, 4, 128), BF)
    natural = pltpu.VMEM((4, 8, 2, 4, 128), BF)
    turned = pltpu.VMEM((8, 4, 2, 4, 128), BF)
    sem = pltpu.SemaphoreType.DMA
    scratch = [
        pltpu.VMEM((1, NEAR), jnp.int32),
        pltpu.VMEM((1, FAR), jnp.int32),
        pltpu.VMEM((EDGE,), jnp.int32),
        pltpu.VMEM((EDGE,), jnp.int32),
        pltpu.VMEM((NODE,), jnp.int32),
        pltpu.VMEM((NODE,), jnp.int32),
        pltpu.VMEM((EXT, D), BF),
        pltpu.VMEM((EDGE, D), BF),
        pltpu.VMEM((NODE, 128), BF),
        pltpu.VMEM((3 * D, D), BF),
        pltpu.VMEM((D, D), BF),
        pltpu.VMEM((2 * D, D), BF),
        pltpu.VMEM((D, D), BF),
        pltpu.VMEM((D, 128), BF),
        near, near, natural, row, near, near, natural, turned, natural,
        pltpu.VMEM((EDGE, TABLE), BF),
        pltpu.VMEM((TABLE, EDGE), BF),
        pltpu.VMEM((NODE, NEAR), BF),
        pltpu.VMEM((NODE, FAR), BF),
        pltpu.VMEM((TABLE, D), BF),
        pltpu.VMEM((EDGE, D), F32),
        pltpu.VMEM((EDGE, D), BF),
        pltpu.VMEM((EDGE, D), BF),
        pltpu.VMEM((EDGE, 128), F32),
        pltpu.VMEM((EDGE, D), BF),
        pltpu.VMEM((EDGE, D), BF),
        pltpu.VMEM((NODE, D), F32),
        pltpu.VMEM((NODE, D), BF),
        pltpu.VMEM((TABLE, D), BF),
        pltpu.VMEM((3 * D, D), F32),
        sem((14,)),
        sem((6,)), sem((6,)), sem((1,)), sem((1,)),
        sem((6,)), sem((6,)), sem((14,)), sem((14,)),
    ] + group_scratch() + group_scratch()
    shapes = (
        jax.ShapeDtypeStruct((1, NODE, D), BF),
        jax.ShapeDtypeStruct((1, EDGE, D), BF),
        jax.ShapeDtypeStruct((24, D), F32),
        jax.ShapeDtypeStruct((8, D), F32),
        jax.ShapeDtypeStruct((16, D), F32),
        jax.ShapeDtypeStruct((8, D), F32),
        jax.ShapeDtypeStruct((8, 128), F32),
    )
    results = pl.pallas_call(
        kernel,
        out_shape=(pltpu.VMEM((1, NODE, D), BF), pltpu.VMEM((1, EDGE, D), BF), pltpu.VMEM((64, D), F32)),
        in_specs=[hbm] * 12 + [pl.BlockSpec(memory_space=pltpu.SMEM)] + [hbm] * 2,
        out_specs=(vmem,) * 3,
        scratch_shapes=scratch,
        compiler_params=pltpu.CompilerParams(
            collective_id=0, has_side_effects=True, vmem_limit_bytes=50 * 1024 * 1024
        ),
    )(*(
        a if a is count else pltpu.with_memory_space_constraint(a, pltpu.HBM)
        for a in args
    ))
    return pl.pallas_call(
        hand_out,
        out_shape=shapes,
        in_specs=[vmem] * 3,
        out_specs=(hbm,) * 7,
        scratch_shapes=[sem((7,))],
        compiler_params=pltpu.CompilerParams(vmem_limit_bytes=3072 * 1024),
    )(*results)


def solution(mesh):
    split = Mesh(
        mesh.devices.reshape(4, 8, 2, mesh.shape["rep"]), ("patch_0", "patch_1", "patch_2", "rep")
    )
    in_specs = (
        P("rep", PATCH, None),
        P("rep", PATCH, None),
        P("rep", PATCH, None),
        P(),
        P(),
        P(),
        P(),
        P(),
        P(PATCH, None),
        P(PATCH, None),
        P(PATCH),
        P(PATCH),
        P(PATCH),
        P(PATCH),
        P(PATCH),
    )
    out_specs = (
        P("rep", PATCH, None),
        P("rep", PATCH, None),
        P(PATCH, None),
        P(PATCH, None),
        P(PATCH, None),
        P(PATCH, None),
        P(PATCH, None),
    )
    return jax.shard_map(body, mesh=split, in_specs=in_specs, out_specs=out_specs, check_vma=False)
```

```python
import functools

import jax
import jax.numpy as jnp
from jax import lax
from jax.experimental import pallas as pl
from jax.experimental.pallas import tpu as pltpu
from jax.sharding import Mesh
from jax.sharding import PartitionSpec as P

OCEAN = 32
BANDS = 721
PATCH = ("patch_0", "patch_1", "patch_2")
MESH = pl.DeviceIdType.MESH
D = 512
NODE = 384
EDGE = 1280
NEAR = 96
FAR = 64
EXT = 640
GOT = EXT - NODE
TABLE = EXT + NODE
TILE = 256
ROWS = 1
OFFSETS = (1, -1, 2, -2, 3, -3)
BF = jnp.bfloat16
F32 = jnp.float32


def dot(a, b):
    return jnp.dot(a, b, preferred_element_type=F32)


def dot_t(a, b):
    return lax.dot_general(a, b, (((1,), (1,)), ((), ())), preferred_element_type=F32)


def t_dot(a, b):
    return lax.dot_general(a, b, (((0,), (0,)), ((), ())), preferred_element_type=F32)


def patch_id(q):
    return {"patch_0": q // 16, "patch_1": (q // 2) % 8, "patch_2": q % 2}


def greet(barrier, device):
    pl.semaphore_signal(barrier, inc=1, device_id=device, device_id_type=MESH)


def normalize(v):
    mean = jnp.mean(v, axis=-1, keepdims=True)
    centred = v - mean
    var = jnp.mean(centred * centred, axis=-1, keepdims=True)
    inverse = lax.rsqrt(var + 1e-05)
    return centred * inverse, inverse


def norm_back(g, y, inverse):
    first = jnp.mean(g, axis=-1, keepdims=True)
    second = jnp.mean(g * y, axis=-1, keepdims=True)
    return inverse * (g - first - y * second)


def columns(rows):
    wide = rows[0].shape[1]
    pad = [jnp.zeros((8 - len(rows), wide), F32)]
    return jnp.concatenate(rows + pad, axis=0).T


class Reducer:
    def __init__(self, refs, where):
        (self.start0, self.r0, self.w1, self.direct, self.relay, self.merged, self.carried,
         self.w2, self.r2, self.w3, self.r3, self.w4, self.r4, self.send, self.recv) = refs
        x, self.y, self.z, self.c = where
        self.axes = ((("patch_0", x), ("rep", self.y)), (("rep", self.y), ("patch_0", x)))
        self.pending = []

    def copy(self, src, dst, k, device):
        one = pltpu.make_async_remote_copy(
            src_ref=src, dst_ref=dst, send_sem=self.send.at[k], recv_sem=self.recv.at[k],
            device_id=device, device_id_type=MESH,
        )
        one.start()
        self.pending.append(one)
        return one

    def pair(self):
        other = 1 - self.c
        self.c0 = [
            self.copy(self.start0.at[h, other], self.r0.at[h], h, {"patch_2": other})
            for h in range(2)
        ]

    def first(self):
        self.c1 = []
        for h in range(2):
            self.c0[h].wait_recv()

            @pl.loop(0, 4)
            def _(i):
                mine = self.start0[h, self.c, i].astype(F32)
                self.w1[h, i] = (mine + self.r0[h, i].astype(F32)).astype(BF)

            axis, at = self.axes[h][0]
            right, left, across = (at + 1) % 4, (at + 3) % 4, (at + 2) % 4
            lo, hi = pl.ds(0, 2), pl.ds(2, 2)
            w1, k = self.w1, 2 + 10 * h
            ends = (right, left)
            relays = [
                self.copy(
                    w1.at[h, across, 2 * side + j], self.relay.at[h, side, j], k + 2 * j + side,
                    {axis: ends[side]},
                )
                for j in range(2)
                for side in range(2)
            ]
            self.c1.append((relays, (
                self.copy(w1.at[h, left, lo], self.direct.at[h, 0], k + 4, {axis: left}),
                self.copy(w1.at[h, right, hi], self.direct.at[h, 1], k + 5, {axis: right}),
            )))

    def middle(self):
        self.c1b = []
        for j in range(2):
            for h in range(2):
                axis, at = self.axes[h][0]
                ends = ((at + 1) % 4, (at + 3) % 4)
                for side in range(2):
                    self.c1[h][0][2 * j + side].wait_recv()
                    mine = self.w1[h, ends[side], 2 * side + j].astype(F32)
                    self.merged[h, side, j] = (mine + self.relay[h, side, j].astype(F32)).astype(BF)
                    self.c1b.append(self.copy(
                        self.merged.at[h, side, j], self.carried.at[h, side, j],
                        8 + 10 * h + 2 * j + side, {axis: ends[side]},
                    ))

    def second(self):
        self.c2 = []
        for h in range(2):
            _, own = self.axes[h][0]
            for side in range(2):
                self.c1[h][1][side].wait_recv()
                for j in range(2):
                    self.c1b[4 * j + 2 * h + side].wait_recv()
                part = pl.ds(2 * side, 2)
                acc = self.w1[h, own, part].astype(F32) + self.direct[h, side].astype(F32)
                self.w2[h, part] = (acc + self.carried[h, side].astype(F32)).astype(BF)
            axis, at = self.axes[h][1]
            for d in range(1, 4):
                to = (at + d) % 4
                self.c2.append(
                    self.copy(self.w2.at[h, to], self.r2.at[h, d - 1], 21 + 3 * h + d, {axis: to})
                )

    def third(self):
        for h in range(2):
            for one in self.c2[3 * h : 3 * h + 3]:
                one.wait_recv()
            acc = self.w2[h, self.axes[h][1][1]].astype(F32)
            for s in range(3):
                acc = acc + self.r2[h, s].astype(F32)
            self.w3[:, h] = acc.astype(BF)
        self.c3 = []
        for d in range(1, 8):
            to = (self.z + d) % 8
            self.c3.append(self.copy(self.w3.at[to], self.r3.at[d - 1], 27 + d, {"patch_1": to}))

    def fourth(self):
        for one in self.c3:
            one.wait_recv()
        acc = self.w3[self.z].astype(F32)
        for s in range(7):
            acc = acc + self.r3[s].astype(F32)
        self.w4[...] = acc * (1.0 / (NODE * 64 * 4))
        self.c4 = []
        for d in range(1, 4):
            to = (self.y + d) % 4
            self.c4.append(self.copy(self.w4, self.r4.at[d - 1], 34 + d, {"rep": to}))

    def last(self):
        for one in self.c4:
            one.wait_recv()
        out = []
        own = self.w4[...]
        got = [self.r4[s] for s in range(3)]
        for y in range(4):
            tile = own
            for s in range(3):
                tile = jnp.where((self.y - s - 1 + 4) % 4 == y, got[s], tile)
            out.append(tile)
        return out

    def finish(self):
        for one in self.pending:
            one.wait_send()


def kernel(
    x_hbm, e_hbm, t_hbm, we_in_hbm, we_out_hbm, wn_in_hbm, wn_out_hbm, wr_hbm,
    send_hbm, far_hbm, sender_hbm, receiver_hbm, count_ref, land_hbm, lat_hbm,
    node_out, edge_out, grads_out,
    send_ref, far_ref, sender_ref, receiver_ref, land_ref, lat_ref,
    xe, e, tgt, we_in, we_out, wn_in, wn_out, wr,
    near_src, near_got, far_src, far_got, back_near_src, back_near_got, back_far_src, back_far_mid, back_far_got,
    onehot, onehot_t, own_near, own_far, proj, pre, hid, msg, inv, ezg, epg, total, agg_grad, gsum, wgrad,
    aggr, node_hid, fresh, nzg, npg, miss, weights,
    *rest,
):
    dma_sem, near_send, near_recv, far_send, far_recv = rest[:5]
    bnear_send, bnear_recv, bfar_send, bfar_recv = rest[5:9]
    group_a, group_b = rest[9:24], rest[24:39]
    ix, iz, ic, iy = (lax.axis_index(a) for a in (*PATCH, "rep"))
    me = ix * 16 + iz * 2 + ic

    loads = {}
    for k, (name, src, dst) in enumerate((
        ("send", send_hbm, send_ref),
        ("far", far_hbm, far_ref),
        ("sender", sender_hbm, sender_ref),
        ("receiver", receiver_hbm, receiver_ref),
        ("x", x_hbm.at[0], xe.at[pl.ds(GOT, NODE)]),
        ("we_in", we_in_hbm, we_in),
        ("e", e_hbm.at[0], e),
        ("we_out", we_out_hbm, we_out),
        ("wn_in", wn_in_hbm, wn_in),
        ("wn_out", wn_out_hbm, wn_out),
        ("wr", wr_hbm, wr),
        ("t", t_hbm.at[0], tgt),
        ("land", land_hbm, land_ref),
        ("lat", lat_hbm, lat_ref),
    )):
        loads[name] = pltpu.make_async_copy(src, dst, dma_sem.at[k])
        if k in (0, 1, 4):
            loads[name].start()

    barrier = pltpu.get_barrier_semaphore()

    xs, zs, cs = ([(i + d) % n for d in range(n)] for i, n in ((ix, 4), (iz, 8), (ic, 2)))
    others = [
        (dx, dz, dc)
        for dx in (2, 1, 3, 0)
        for dz in (4, 3, 5, 2, 6, 1, 7, 0)
        for dc in range(2)
        if dx or dz or dc
    ]
    for dx, dz, dc in others:
        greet(barrier, {"patch_0": xs[dx], "patch_1": zs[dz], "patch_2": cs[dc]})

    for d in range(1, 4):
        greet(barrier, {"rep": (iy + d) % 4})

    for name in loads:
        if name not in ("send", "far", "x"):
            loads[name].start()

    loads["send"].wait()
    loads["far"].wait()
    ids = lax.broadcasted_iota(jnp.int32, (NODE, NEAR), 0)
    own_near[...] = jnp.where(ids == send_ref[...], 1.0, 0.0).astype(BF)
    ids = lax.broadcasted_iota(jnp.int32, (NODE, FAR), 0)
    own_far[...] = jnp.where(ids == far_ref[...], 1.0, 0.0).astype(BF)
    loads["x"].wait()
    x = xe[pl.ds(GOT, NODE), :]
    near_src[...] = t_dot(own_near[...], x).astype(BF).reshape(6, 16, D)
    far_src[...] = t_dot(own_far[...], x).astype(BF).reshape(4, 8, 2, 4, 128)

    pl.semaphore_wait(barrier, 66)

    nears = []
    for k, o in enumerate(OFFSETS):
        one = pltpu.make_async_remote_copy(
            src_ref=near_src.at[k], dst_ref=near_got.at[k],
            send_sem=near_send.at[k], recv_sem=near_recv.at[k],
            device_id=patch_id((me + o + 64) % 64), device_id_type=MESH,
        )
        one.start()
        nears.append(one)

    def remote(src, dst, sems, k, device):
        one = pltpu.make_async_remote_copy(
            src_ref=src, dst_ref=dst, send_sem=sems[0].at[k], recv_sem=sems[1].at[k],
            device_id=device, device_id_type=MESH,
        )
        one.start()
        return one

    def plane(k):
        return {"patch_0": k // 2, "patch_2": k % 2}

    for dx, dz, dc in others:
        pltpu.make_async_remote_copy(
            src_ref=far_src.at[xs[dx], zs[dz], cs[dc]], dst_ref=far_got.at[me],
            send_sem=far_send.at[0], recv_sem=far_recv.at[0],
            device_id={"patch_0": xs[dx], "patch_1": zs[dz], "patch_2": cs[dc]},
            device_id_type=MESH,
        ).start()

    far_all = pltpu.make_async_remote_copy(
        src_ref=far_got.at[pl.ds(0, 63)], dst_ref=far_got.at[pl.ds(0, 63)],
        send_sem=far_send.at[0], recv_sem=far_recv.at[0],
        device_id=patch_id((me + 1) % 64), device_id_type=MESH,
    )

    spot = lax.broadcasted_iota(jnp.int32, (1, EDGE), 1)
    live = spot < count_ref[0]
    loads["sender"].wait()
    loads["receiver"].wait()
    s_row = sender_ref[...].reshape(1, EDGE)
    s_row = jnp.where(live, jnp.where(s_row < NODE, s_row + GOT, s_row - NODE), -1)
    r_row = jnp.where(live, receiver_ref[...].reshape(1, EDGE) + EXT, -1)
    cols = columns([s_row.astype(F32), r_row.astype(F32)])
    s_col = cols[:, 0:1].astype(jnp.int32)
    r_col = cols[:, 1:2].astype(jnp.int32)
    for k in range(TABLE // 128):
        ids = lax.broadcasted_iota(jnp.int32, (EDGE, 128), 1) + k * 128
        which = s_col if k < EXT // 128 else r_col
        onehot[:, pl.ds(k * 128, 128)] = jnp.where(ids == which, 1.0, 0.0).astype(BF)
    for k in range(TABLE // 128):
        ids = lax.broadcasted_iota(jnp.int32, (128, EDGE), 0) + k * 128
        which = s_row if k < EXT // 128 else r_row
        onehot_t[pl.ds(k * 128, 128), :] = jnp.where(ids == which, 1.0, 0.0).astype(BF)

    loads["we_in"].wait()
    proj[pl.ds(GOT, NODE), :] = dot(x, we_in[pl.ds(0, D), :]).astype(BF)
    proj[pl.ds(EXT, NODE), :] = dot(x, we_in[pl.ds(D, D), :]).astype(BF)
    loads["e"].wait()
    pre[...] = dot(e[...], we_in[pl.ds(2 * D, D), :]) + dot(
        onehot[:, pl.ds(GOT, 2 * NODE)], proj[pl.ds(GOT, 2 * NODE), :]
    )

    loads["land"].wait()
    loads["lat"].wait()
    latitude = -0.5 * jnp.pi + (lat_ref[...].reshape(1, NODE).astype(F32) + 0.5) * (jnp.pi / BANDS)
    cols = columns([jnp.cos(latitude), land_ref[...].reshape(1, NODE).astype(F32)])
    channel = lax.broadcasted_iota(jnp.int32, (NODE, 128), 1)
    weights[...] = jnp.where((channel < OCEAN) & (cols[:, 1:2] == 1.0), 0.0, cols[:, 0:1])
    loads["wn_in"].wait()
    total[...] = dot(x, wn_in[pl.ds(0, D), :])
    for one in nears:
        one.wait_recv()
    far_all.wait_recv()
    xe[pl.ds(0, NEAR), :] = near_got[...].reshape(NEAR, D)
    slot = lax.broadcasted_iota(jnp.int32, (FAR, 4, 128), 0)
    far_rows = jnp.where(slot == me, far_src[...].reshape(FAR, 4, 128), far_got[...]).reshape(FAR, D)
    xe[pl.ds(NEAR, FAR), :] = far_rows
    xe[pl.ds(NEAR + FAR, 96), :] = jnp.zeros((96, D), BF)
    proj[pl.ds(0, GOT), :] = dot(xe[pl.ds(0, GOT), :], we_in[pl.ds(0, D), :]).astype(BF)

    loads["we_out"].wait()

    count = EDGE // TILE
    tiles = [pl.ds(k * TILE, TILE) for k in range(count)]

    def enter(k):
        return pre[tiles[k], :] + dot(onehot[tiles[k], pl.ds(0, GOT)], proj[pl.ds(0, GOT), :])

    def activate(k, v):
        s = jax.nn.sigmoid(v)
        h = (v * s).astype(BF)
        hid[tiles[k], :] = h
        pre[tiles[k], :] = s * (1.0 + v * (1.0 - s))
        return dot(h, we_out[...])

    def settle(k, out):
        normed, inverse = normalize(out)
        msg[tiles[k], :] = normed.astype(BF)
        inv[tiles[k], :] = jnp.broadcast_to(inverse, (TILE, 128))

    v, out = enter(0), None
    for k in range(count):
        v_next = enter(k + 1) if k + 1 < count else None
        out_next = activate(k, v)
        if out is not None:
            settle(k - 1, out)
        v, out = v_next, out_next
    settle(count - 1, out)

    aggregate = dot(onehot_t[pl.ds(EXT, NODE), :], msg[...]).astype(BF)

    aggr[...] = aggregate
    span = NODE // ROWS
    parts = [pl.ds(k * span, span) for k in range(ROWS)]
    loads["wn_out"].wait()
    loads["wr"].wait()
    loads["t"].wait()
    def bend(p):
        node_pre = total[p, :] + dot(aggr[p, :], wn_in[pl.ds(D, D), :])
        s = jax.nn.sigmoid(node_pre)
        node_hid[p, :] = (node_pre * s).astype(BF)
        return s * (1.0 + node_pre * (1.0 - s))

    def lift(p):
        normed, inverse = normalize(dot(node_hid[p, :], wn_out[...]))
        fresh[p, :] = (xe[pl.ds(GOT + p.start, span), :].astype(F32) + normed).astype(BF)
        return normed, inverse

    def judge(p):
        weight = weights[p, :]
        grad = weight * (dot(fresh[p, :], wr[...]) - tgt[p, :].astype(F32))
        miss[p, :] = grad.astype(BF)
        return dot_t(miss[p, :], wr[...])

    def lower(p, grad, normed, inverse):
        nzg[p, :] = norm_back(grad, normed, inverse).astype(BF)
        return dot_t(nzg[p, :], wn_out[...])

    slopes = [bend(p) for p in parts]
    norms = [lift(p) for p in parts]
    grads = [judge(p) for p in parts]
    downs = [lower(p, g, *n) for p, g, n in zip(parts, grads, norms)]
    for p, down, slope in zip(parts, downs, slopes):
        npg[p, :] = (down * slope).astype(BF)
    for p, grad in zip(parts, grads):
        aggregate_grad = dot_t(npg[p, :], wn_in[pl.ds(D, D), :])
        centre = jnp.mean(aggregate_grad, axis=-1, keepdims=True)
        agg_grad[p, :] = (aggregate_grad - centre).astype(BF)
        total[p, :] = grad + dot_t(npg[p, :], wn_in[pl.ds(0, D), :])

    where = (ix, iy, iz, ic)
    ga, gb = Reducer(group_a, where), Reducer(group_b, where)

    def pack_rows(start0, value, blocks, slots):
        rows = value.reshape(4, 8, 2, blocks, 8, D)
        for b, (h, t) in enumerate(slots):
            for c in range(2):
                for y in range(4):
                    tile = rows[:, :, c, b, :, y * 128 : (y + 1) * 128].astype(BF)
                    if h == 0:
                        start0[h, c, :, y, :, t] = tile
                    else:
                        start0[h, c, y, :, :, t] = tile

    wgrad[pl.ds(0, D), :] = t_dot(x, npg[...])
    wgrad[pl.ds(D, D), :] = t_dot(aggr[...], npg[...])
    pack_rows(ga.start0, wgrad[pl.ds(0, 2 * D), :], 2, ((0, 0), (0, 1)))
    pack_rows(ga.start0, t_dot(node_hid[...], nzg[...]), 1, ((1, 0),))
    readout = t_dot(fresh[...], miss[...]).reshape(4, 8, 2, 8, 128)
    for c in range(2):
        for y in range(4):
            ga.start0[1, c, y, :, :, 1] = readout[:, :, c].astype(BF)
    ga.pair()

    def gather(k):
        return dot(onehot[tiles[k], pl.ds(EXT, NODE)], agg_grad[...])

    def norm_step(k, g):
        y = msg[tiles[k], :].astype(F32)
        second = jnp.mean(g * y, axis=-1, keepdims=True)
        z_grad = (inv[tiles[k], :][:, 0:1] * (g - y * second)).astype(BF)
        ezg[tiles[k], :] = z_grad
        return dot_t(z_grad, we_out[...])

    def slope_step(k, out):
        epg[tiles[k], :] = (out * pre[tiles[k], :]).astype(BF)

    g, out = gather(0), None
    for k in range(count):
        g_next = gather(k + 1) if k + 1 < count else None
        out_next = norm_step(k, g)
        if out is not None:
            slope_step(k - 1, out)
        g, out = g_next, out_next
        if k == (count + 1) // 2 - 1:
            ga.first()
    slope_step(count - 1, out)

    gsum[...] = dot(onehot_t[...], epg[...]).astype(BF)

    wgrad[pl.ds(2 * D, D), :] = t_dot(e[...], epg[...])
    pack_rows(gb.start0, t_dot(hid[...], ezg[...]), 1, ((1, 1),))
    ga.middle()
    wgrad[pl.ds(0, D), :] = t_dot(xe[...], gsum[pl.ds(0, EXT), :])
    wgrad[pl.ds(D, D), :] = t_dot(x, gsum[pl.ds(EXT, NODE), :])
    pack_rows(gb.start0, wgrad[...], 3, ((0, 0), (0, 1), (1, 0)))
    gb.pair()
    back = dot_t(gsum[pl.ds(0, GOT), :], we_in[pl.ds(0, D), :])
    back_near_src[...] = back[0:NEAR].astype(BF).reshape(6, 16, D)
    back_far_src[...] = back[NEAR : NEAR + FAR].astype(BF).reshape(4, 8, 2, 4, 128)
    backs = []
    for k, o in enumerate(OFFSETS):
        one = pltpu.make_async_remote_copy(
            src_ref=back_near_src.at[k], dst_ref=back_near_got.at[k],
            send_sem=bnear_send.at[k], recv_sem=bnear_recv.at[k],
            device_id=patch_id((me - o + 64) % 64), device_id_type=MESH,
        )
        one.start()
        backs.append(one)

    spot_xc = ix * 2 + ic
    bfars = []

    def remote(src, dst, sems, k, device):
        one = pltpu.make_async_remote_copy(
            src_ref=src, dst_ref=dst, send_sem=sems[0].at[k], recv_sem=sems[1].at[k],
            device_id=device, device_id_type=MESH,
        )
        one.start()
        return one

    for d in range(1, 8):
        to = (iz + d) % 8
        bfars.append(remote(
            back_far_src.at[:, to], back_far_mid.at[iz], (bfar_send, bfar_recv), d - 1,
            {"patch_1": to},
        ))
    back_far_mid[pl.ds(iz, 1)] = back_far_src[:, pl.ds(iz, 1)].reshape(1, 4, 2, 4, 128)

    edge_out[0] = dot_t(epg[...], we_in[pl.ds(2 * D, D), :]).astype(BF)
    gb.first()
    ga.second()
    total[...] += dot_t(gsum[pl.ds(GOT, NODE), :], we_in[pl.ds(0, D), :]) + dot_t(
        gsum[pl.ds(EXT, NODE), :], we_in[pl.ds(D, D), :]
    )
    gb.middle()

    for one in bfars:
        one.wait_recv()
    for d in range(1, 8):
        to = (spot_xc + d) % 8
        bfars.append(remote(
            back_far_mid.at[:, to // 2, to % 2], back_far_got.at[ix, :, ic],
            (bfar_send, bfar_recv), 6 + d, {"patch_0": to // 2, "patch_2": to % 2},
        ))
    back_far_got[pl.ds(ix, 1), :, pl.ds(ic, 1)] = back_far_mid[
        :, pl.ds(ix, 1), pl.ds(ic, 1)
    ].reshape(1, 8, 1, 4, 128)
    gb.second()
    ga.third()

    for one in backs + bfars[7:]:
        one.wait_recv()
    far_rows = back_far_got[...].reshape(FAR, D)
    owned = dot(own_near[...], back_near_got[...].reshape(NEAR, D)) + dot(own_far[...], far_rows)
    node_out[0] = (total[...] + owned).astype(BF)

    gb.third()
    ga.fourth()
    gb.fourth()
    parts = ga.last()
    for y in range(4):
        at = pl.ds(y * 128, 128)
        grads_out[pl.ds(32, 8), at] = parts[y][0, 0]
        grads_out[pl.ds(40, 8), at] = parts[y][0, 1]
        grads_out[pl.ds(48, 8), at] = parts[y][1, 0]
    grads_out[pl.ds(56, 8), pl.ds(0, 128)] = parts[0][1, 1]
    grads_out[pl.ds(56, 8), pl.ds(128, 384)] = jnp.zeros((8, 384), F32)
    parts = gb.last()
    for y in range(4):
        at = pl.ds(y * 128, 128)
        grads_out[pl.ds(0, 8), at] = parts[y][0, 0]
        grads_out[pl.ds(8, 8), at] = parts[y][0, 1]
        grads_out[pl.ds(16, 8), at] = parts[y][1, 0]
        grads_out[pl.ds(24, 8), at] = parts[y][1, 1]

    for one in nears + backs + bfars:
        one.wait_send()
    far_all.wait_send()
    ga.finish()
    gb.finish()


def hand_out(node, edge, grads, *rest):
    outs, sems = rest[:7], rest[7]
    parts = ((0, 24, D), (24, 8, D), (32, 16, D), (48, 8, D), (56, 8, 128))
    moves = [(edge, outs[1]), (node, outs[0])] + [
        (grads.at[pl.ds(at, n), pl.ds(0, w)], outs[2 + k]) for k, (at, n, w) in enumerate(parts)
    ]
    gives = [pltpu.make_async_copy(src, dst, sems.at[k]) for k, (src, dst) in enumerate(moves)]
    for one in gives:
        one.start()
    for one in gives:
        one.wait()


def group_scratch():
    tail = (8, 128)
    return [
        pltpu.VMEM((2, 2, 4, 4, 8, 2, *tail), BF),
        pltpu.VMEM((2, 4, 4, 8, 2, *tail), BF),
        pltpu.VMEM((2, 4, 4, 8, 2, *tail), BF),
        pltpu.VMEM((2, 2, 2, 8, 2, *tail), BF),
        pltpu.VMEM((2, 2, 2, 8, 2, *tail), BF),
        pltpu.VMEM((2, 2, 2, 8, 2, *tail), BF),
        pltpu.VMEM((2, 2, 2, 8, 2, *tail), BF),
        pltpu.VMEM((2, 4, 8, 2, *tail), BF),
        pltpu.VMEM((2, 3, 8, 2, *tail), BF),
        pltpu.VMEM((8, 2, 2, *tail), BF),
        pltpu.VMEM((7, 2, 2, *tail), BF),
        pltpu.VMEM((2, 2, *tail), F32),
        pltpu.VMEM((3, 2, 2, *tail), F32),
        pltpu.SemaphoreType.DMA((38,)),
        pltpu.SemaphoreType.DMA((38,)),
    ]


def body(*args):
    (x, e, t, we_in, we_out, wn_in, wn_out, wr, send, far, sender, receiver, count, land, lat) = args
    hbm = pl.BlockSpec(memory_space=pltpu.HBM)
    vmem = pl.BlockSpec(memory_space=pltpu.VMEM)
    near = pltpu.VMEM((6, 16, D), BF)
    node = pltpu.VMEM((NODE, D), BF)
    row = pltpu.VMEM((FAR, 4, 128), BF)
    natural = pltpu.VMEM((4, 8, 2, 4, 128), BF)
    turned = pltpu.VMEM((8, 4, 2, 4, 128), BF)
    sem = pltpu.SemaphoreType.DMA
    scratch = [
        pltpu.VMEM((1, NEAR), jnp.int32),
        pltpu.VMEM((1, FAR), jnp.int32),
        pltpu.VMEM((EDGE,), jnp.int32),
        pltpu.VMEM((EDGE,), jnp.int32),
        pltpu.VMEM((NODE,), jnp.int32),
        pltpu.VMEM((NODE,), jnp.int32),
        pltpu.VMEM((EXT, D), BF),
        pltpu.VMEM((EDGE, D), BF),
        pltpu.VMEM((NODE, 128), BF),
        pltpu.VMEM((3 * D, D), BF),
        pltpu.VMEM((D, D), BF),
        pltpu.VMEM((2 * D, D), BF),
        pltpu.VMEM((D, D), BF),
        pltpu.VMEM((D, 128), BF),
        near, near, natural, row, near, near, natural, turned, natural,
        pltpu.VMEM((EDGE, TABLE), BF),
        pltpu.VMEM((TABLE, EDGE), BF),
        pltpu.VMEM((NODE, NEAR), BF),
        pltpu.VMEM((NODE, FAR), BF),
        pltpu.VMEM((TABLE, D), BF),
        pltpu.VMEM((EDGE, D), F32),
        pltpu.VMEM((EDGE, D), BF),
        pltpu.VMEM((EDGE, D), BF),
        pltpu.VMEM((EDGE, 128), F32),
        pltpu.VMEM((EDGE, D), BF),
        pltpu.VMEM((EDGE, D), BF),
        pltpu.VMEM((NODE, D), F32),
        pltpu.VMEM((NODE, D), BF),
        pltpu.VMEM((TABLE, D), BF),
        pltpu.VMEM((3 * D, D), F32),
        node, node, node, node, node, pltpu.VMEM((NODE, 128), BF), pltpu.VMEM((NODE, 128), F32),
        sem((14,)),
        sem((6,)), sem((6,)), sem((1,)), sem((1,)),
        sem((6,)), sem((6,)), sem((14,)), sem((14,)),
    ] + group_scratch() + group_scratch()
    shapes = (
        jax.ShapeDtypeStruct((1, NODE, D), BF),
        jax.ShapeDtypeStruct((1, EDGE, D), BF),
        jax.ShapeDtypeStruct((24, D), F32),
        jax.ShapeDtypeStruct((8, D), F32),
        jax.ShapeDtypeStruct((16, D), F32),
        jax.ShapeDtypeStruct((8, D), F32),
        jax.ShapeDtypeStruct((8, 128), F32),
    )
    results = pl.pallas_call(
        kernel,
        out_shape=(pltpu.VMEM((1, NODE, D), BF), pltpu.VMEM((1, EDGE, D), BF), pltpu.VMEM((64, D), F32)),
        in_specs=[hbm] * 12 + [pl.BlockSpec(memory_space=pltpu.SMEM)] + [hbm] * 2,
        out_specs=(vmem,) * 3,
        scratch_shapes=scratch,
        compiler_params=pltpu.CompilerParams(
            collective_id=0, has_side_effects=True, vmem_limit_bytes=50 * 1024 * 1024
        ),
    )(*(
        a if a is count else pltpu.with_memory_space_constraint(a, pltpu.HBM)
        for a in args
    ))
    return pl.pallas_call(
        hand_out,
        out_shape=shapes,
        in_specs=[vmem] * 3,
        out_specs=(hbm,) * 7,
        scratch_shapes=[sem((7,))],
        compiler_params=pltpu.CompilerParams(vmem_limit_bytes=3072 * 1024),
    )(*results)


def solution(mesh):
    split = Mesh(
        mesh.devices.reshape(4, 8, 2, mesh.shape["rep"]), ("patch_0", "patch_1", "patch_2", "rep")
    )
    in_specs = (
        P("rep", PATCH, None),
        P("rep", PATCH, None),
        P("rep", PATCH, None),
        P(),
        P(),
        P(),
        P(),
        P(),
        P(PATCH, None),
        P(PATCH, None),
        P(PATCH),
        P(PATCH),
        P(PATCH),
        P(PATCH),
        P(PATCH),
    )
    out_specs = (
        P("rep", PATCH, None),
        P("rep", PATCH, None),
        P(PATCH, None),
        P(PATCH, None),
        P(PATCH, None),
        P(PATCH, None),
        P(PATCH, None),
    )
    return jax.shard_map(body, mesh=split, in_specs=in_specs, out_specs=out_specs, check_vma=False)
```
